32 devices in a mesh: span: 2 (over y), height: 4 (over x, core), depth: 4 (over z).
Axes of the slice: x: 2, y: 2, z: 4, core: 2. Of those that a mesh axis runs over, the one named last changes fastest.
Arguments:
- load: float32 [8, 32, 64, 512], P(None, 'span', 'height', 'depth'), may hold values from -6 to 6
- phase: float32 [32, 64, 512], P('span', 'height', 'depth'), may hold values from 0.1 to 1
- void: int32 [4, 8, 64], P('span', 'height', 'depth'), may hold values from 0 to 1, as said below
- owner: int32 [4, 8, 64], P('span', 'height', 'depth'), may hold values from 0 to 1, as said below
- precond: bfloat16 [512, 512, 512], P(('span', 'height', 'depth')), may hold values from -1 to 2, as said below
Outputs:
- displacement: float32 [8, 32, 64, 512], P(None, 'span', 'height', 'depth')
- sensitivity: float32 [32, 64, 512], P('span', 'height', 'depth')
- phase_next: float32 [32, 64, 512], P('span', 'height', 'depth')
The draws below stay inside these ranges and needn't reach their ends.
Inputs may be any that keep to these rules, and one draw needn't show every extreme that they name: `void`: each device's block of 16 x 16 x 128 cells holds at most 16 solid bricks; some device holds exactly 16. `owner`: among the solid bricks of one device at most 8 name any one value; on some device every value is named by exactly 8 solid bricks. Values of void bricks carry no meaning. `precond`: every block is symmetric with a positive diagonal that dominates each row.
All inputs are finite; a program needn't handle non-finite values.
Results may differ from the reference program's by a relative error of at most 0.0021.
Values may be sent and summed in bfloat16 or wider, within the bound.
No kernel may reach another device: no remote copies, remote signals or barrier semaphores. Data moves between devices by JAX's collectives and lax.ppermute only.
A program may use at most 128 MiB of HBM per device.

```python
import jax
import jax.numpy as jnp
from jax import lax

BE = 8
CX = 16
CY = 16
CZ = 128
NLOAD = 8
ITERS = 2
SWEEPS = 2
BC = 512
NBD = 64
OWN = 16
CAP = 8
SLOTS = 512
NX = 32
NY = 64
NZ = 512
N_SPAN = 2
N_HEIGHT = 4
N_DEPTH = 4


def brick_plan(key):
    key = jax.random.fold_in(key, 7)
    span_count = NX // CX
    height_count = NY // CY
    depth_count = NZ // CZ
    device_count = span_count * height_count * depth_count
    capacity = OWN // span_count
    first, second, third, fourth = jax.random.split(key, 4)
    counts = jax.random.randint(first, (device_count,), OWN // 4, OWN + 1)
    chosen = jax.random.randint(second, (), 0, device_count)
    counts = jnp.where(jnp.arange(device_count) == chosen, OWN, counts)
    scores = jax.random.randint(third, (device_count, NBD), 0, 1 << 20) * NBD + jnp.arange(NBD, dtype=jnp.int32)[None, :]
    ordering = jnp.argsort(scores, axis=1)
    position = jnp.argsort(ordering, axis=1)
    solid = (position < counts[:, None]).astype(jnp.int32)
    before = jnp.cumsum(solid, axis=1) - solid
    offsets = jax.random.randint(fourth, (device_count,), 0, span_count)
    span_index = jnp.arange(device_count, dtype=jnp.int32) // (height_count * depth_count)
    owners = (span_index[:, None] + offsets[:, None] + before // capacity) % span_count

    def to_grid(values):
        g = values.reshape(span_count, height_count, depth_count, CX // BE, CY // BE, CZ // BE)
        g = g.transpose(0, 3, 1, 4, 2, 5)
        return g.reshape(NX // BE, NY // BE, NZ // BE).astype(jnp.int32)
    return (to_grid(1 - solid), to_grid(owners))


def draw_void(key, part):
    return brick_plan(key)[0]


def draw_owner(key, part):
    return brick_plan(key)[1]


def draw_precond(key, part):
    key = jax.random.fold_in(key, 11)

    def one_block(index):
        block_key = jax.random.fold_in(key, index)
        first, second = jax.random.split(block_key)
        raw = jax.random.normal(first, (BC, BC), jnp.float32) * (0.9 / BC)
        symmetric = 0.5 * (raw + raw.T)
        diagonal = jax.random.uniform(second, (BC,), jnp.float32, 1.0, 2.0)
        identity = jnp.eye(BC, dtype=jnp.float32)
        return (symmetric * (1.0 - identity) + diagonal[:, None] * identity).astype(jnp.bfloat16)
    return jax.lax.map(one_block, jnp.arange(SLOTS, dtype=jnp.int32))


def steps_of(rng, shape, shards, smallest, top_value):
    factor_of = 1.0
    for dim, shards_of in shards:
        steps = jax.random.uniform(jax.random.fold_in(jax.random.fold_in(rng, 6), dim), (shards_of,), jnp.float32, smallest / len(shards), top_value / len(shards))
        factor_of = factor_of * jnp.repeat(jnp.exp(steps), shape[dim] // shards_of).reshape((-1,) + (1,) * (len(shape) - 1 - dim))
    return factor_of


def gaussian(key, dims, scale, reach, cuts=(), kind=jnp.bfloat16):
    entries = scale * jax.random.normal(key, dims, jnp.float32)
    if cuts:
        entries = entries * steps_of(key, dims, cuts, -0.22, 0.18)
    return jnp.clip(entries, -reach, reach).astype(kind)


def setup_inputs(seed: int = 0) -> dict:
    streams_of = jax.random.split(jax.random.key(seed), 6)
    load = gaussian(streams_of[0], (NLOAD, NX, NY, NZ), 1.0, 6.0, ((1, 2), (2, 4), (3, 4)), jnp.float32)
    phase = jnp.clip(0.1 + 0.9 * jax.random.uniform(streams_of[1], (NX, NY, NZ), jnp.float32) ** steps_of(streams_of[1], (NX, NY, NZ), ((0, 2), (1, 4), (2, 4)), -0.2, 0.2), 0.1, 1.0)
    void = draw_void(jax.random.fold_in(streams_of[5], 71), 0)
    owner = draw_owner(jax.random.fold_in(streams_of[5], 71), 0)
    precond = draw_precond(jax.random.fold_in(streams_of[5], 71), 0)
    return {"load": load, "phase": phase, "void": void, "owner": owner, "precond": precond}


void_stiffness = 0.001
spring_rate = 0.05
time_step = 0.5
interface_weight = 0.5
epsilon_peak = 1e-6


def pad_three(field):
    return jnp.pad(field, [(0, 0)] * (field.ndim - 3) + [(1, 1)] * 3)


def neighbours(padded):
    return [padded[..., 2:, 1:-1, 1:-1], padded[..., :-2, 1:-1, 1:-1],
            padded[..., 1:-1, 2:, 1:-1], padded[..., 1:-1, :-2, 1:-1],
            padded[..., 1:-1, 1:-1, 2:], padded[..., 1:-1, 1:-1, :-2]]


def cells_of(bricks):
    expanded = jnp.broadcast_to(bricks[:, None, :, None, :, None], (bricks.shape[0], BE, bricks.shape[1], BE, bricks.shape[2], BE))
    return expanded.reshape(bricks.shape[0] * BE, bricks.shape[1] * BE, bricks.shape[2] * BE)


def local_order(grid):
    g = grid.reshape(N_SPAN, CX // BE, N_HEIGHT, CY // BE, N_DEPTH, CZ // BE).transpose(0, 2, 4, 1, 3, 5)
    return g.reshape(N_SPAN * N_HEIGHT * N_DEPTH, NBD)


def to_device_bricks(field):
    loads = field.shape[0]
    f = field.reshape(loads, N_SPAN, CX // BE, BE, N_HEIGHT, CY // BE, BE, N_DEPTH, CZ // BE, BE)
    f = f.transpose(1, 4, 7, 2, 5, 8, 0, 3, 6, 9)
    return f.reshape(N_SPAN * N_HEIGHT * N_DEPTH * NBD, loads, BC)


def from_device_bricks(bricks):
    loads = bricks.shape[1]
    f = bricks.reshape(N_SPAN, N_HEIGHT, N_DEPTH, CX // BE, CY // BE, CZ // BE, loads, BE, BE, BE)
    f = f.transpose(6, 0, 3, 7, 1, 4, 8, 2, 5, 9)
    return f.reshape(loads, NX, NY, NZ)


def slot_table(void, owner):
    solid = 1 - local_order(void)
    owned = local_order(owner)
    columns = jnp.arange(N_SPAN, dtype=jnp.int32)
    onehot = (owned[:, :, None] == columns[None, None, :]).astype(jnp.int32) * solid[:, :, None]
    before = jnp.cumsum(onehot, axis=1) - onehot
    rank = jnp.sum(before * onehot, axis=2)
    device_ids = jnp.arange(N_SPAN * N_HEIGHT * N_DEPTH, dtype=jnp.int32)
    cross = device_ids % (N_HEIGHT * N_DEPTH)
    source = device_ids // (N_HEIGHT * N_DEPTH)
    owner_device = owned * (N_HEIGHT * N_DEPTH) + cross[:, None]
    slot = owner_device * OWN + source[:, None] * CAP + rank
    slot = jnp.where(solid == 1, slot, SLOTS).astype(jnp.int32)
    return slot.reshape(-1), solid.reshape(-1)


def precondition(residual, precond, slot, solid):
    bricks = to_device_bricks(residual.astype(jnp.bfloat16))
    loads = bricks.shape[1]
    filled = jnp.zeros((SLOTS, loads, BC), jnp.bfloat16).at[slot].set(bricks, mode="drop")
    blocks = precond.reshape(N_SPAN * N_HEIGHT * N_DEPTH, OWN, BC, BC)
    inputs = filled.reshape(N_SPAN * N_HEIGHT * N_DEPTH, OWN, loads, BC)

    def apply_device(pair):
        return jnp.einsum("sij,slj->sli", pair[0].astype(jnp.float32), pair[1].astype(jnp.float32))

    images = lax.map(apply_device, (blocks, inputs)).reshape(SLOTS, loads, BC)
    safe = jnp.minimum(slot, SLOTS - 1).astype(jnp.int32)
    result = images[safe] * solid.astype(jnp.float32)[:, None, None]
    return from_device_bricks(result)


def reference(load, phase, void, owner, precond):
    cell_mask = cells_of((1 - void).astype(jnp.float32))
    stiffness = void_stiffness + (1.0 - void_stiffness) * phase ** 3
    near_mask = neighbours(pad_three(cell_mask))
    near_stiff = neighbours(pad_three(cell_mask * stiffness))
    weights = [cell_mask * 0.5 * (nm * stiffness + nk) for nm, nk in zip(near_mask, near_stiff)]

    def operate(field):
        total = cell_mask * spring_rate * field
        for weight, near in zip(weights, neighbours(pad_three(field))):
            total = total + weight * (field - near)
        return total

    slot, solid = slot_table(void, owner)
    right_side = cell_mask[None] * load
    solution = jnp.zeros_like(right_side)
    residual = right_side
    search = precondition(residual, precond, slot, solid)
    norm_now = jnp.sum(residual * search, axis=(1, 2, 3))
    direction = search
    for iteration in range(ITERS):
        image = operate(direction)
        step_size = norm_now / jnp.sum(direction * image, axis=(1, 2, 3))
        solution = solution + step_size[:, None, None, None] * direction
        residual = residual - step_size[:, None, None, None] * image
        if iteration + 1 < ITERS:
            search = precondition(residual, precond, slot, solid)
            norm_next = jnp.sum(residual * search, axis=(1, 2, 3))
            direction = search + (norm_next / norm_now)[:, None, None, None] * direction
            norm_now = norm_next
    energy = jnp.zeros_like(phase)
    for mask_near, near in zip(near_mask, neighbours(pad_three(solution))):
        energy = energy + mask_near * jnp.sum((solution - near) ** 2, axis=0)
    sensitivity = -1.5 * (1.0 - void_stiffness) * phase ** 2 * cell_mask * energy
    peak_value = jnp.max(-sensitivity)
    drive = phase / time_step - 0.5 * phase * (1.0 - phase) * (1.0 - 2.0 * phase) - sensitivity / (peak_value + epsilon_peak)
    inverse = 1.0 / (1.0 / time_step + 6.0 * interface_weight)
    current = phase
    for sweep_index in range(SWEEPS):
        beside_all = neighbours(pad_three(current))
        current = (drive + interface_weight * (beside_all[0] + beside_all[1] + beside_all[2] + beside_all[3] + beside_all[4] + beside_all[5])) * inverse
    return solution, sensitivity, current
```

```python
import jax
import jax.numpy as jnp
from jax import lax
from jax.experimental import pallas as pl
from jax.experimental.pallas import tpu as pltpu
from jax.sharding import PartitionSpec as P

BE = 8
AXES = ("span", "height", "depth")

void_stiffness = 0.001
spring_rate = 0.05
time_step = 0.5
interface_weight = 0.5
epsilon_peak = 1e-06
inverse = 1.0 / (1.0 / time_step + 6.0 * interface_weight)

F32 = jnp.float32
BF16 = jnp.bfloat16
VM = pl.BlockSpec(memory_space=pltpu.VMEM)
SM = pl.BlockSpec(memory_space=pltpu.SMEM)


def call(kernel, ins, outs, scratch=(), aliases=None, flops=0, name=None):
    return pl.pallas_call(
        kernel,
        in_specs=[spec for _, spec in ins],
        out_specs=[spec for _, _, spec in outs],
        out_shape=[jax.ShapeDtypeStruct(shape, dtype) for shape, dtype, _ in outs],
        scratch_shapes=list(scratch),
        input_output_aliases=aliases or {},
        cost_estimate=pl.CostEstimate(flops=flops, bytes_accessed=1 << 20, transcendentals=0),
        name=name,
    )(*[array for array, _ in ins])


def local(load, phase, void, owner, precond):
    loads, X, Y, Z = load.shape
    bricks_x, bricks_y, bricks_z = void.shape
    bricks = bricks_x * bricks_y * bricks_z
    T = Y // BE
    tiles = X * T
    cells = BE**3
    lanes = Z
    assert lanes == 128 and BE == 8 and lanes % tiles == 0
    per_pack = lanes // tiles
    packs = -(-loads // per_pack)
    assert loads % per_pack == 0 and per_pack >= 2
    sizes = [lax.axis_size(axis) for axis in AXES]
    assert all(size % 2 == 0 for size in sizes)
    spans = sizes[0]
    devices = sizes[0] * sizes[1] * sizes[2]
    slots = precond.shape[0]
    cap = slots // spans
    bits = 32 // spans
    assert cap < (1 << min(bits, 8)) and bits >= 2
    remote = (spans - 1) * cap

    coords = jnp.stack([lax.axis_index(axis) for axis in AXES]).astype(jnp.int32)
    load_f = load.reshape(loads, X * Y, Z)
    phase_f = phase.reshape(X * Y, Z)
    void_f = void.reshape(bricks)
    owner_f = owner.reshape(bricks)

    def iotas():
        return (
            lax.broadcasted_iota(jnp.int32, (8, lanes), 0),
            lax.broadcasted_iota(jnp.int32, (8, lanes), 1),
        )

    def row(x, t):
        start = x * Y + t * 8
        return pl.ds(start if isinstance(start, int) else pl.multiple_of(start, 8), 8)

    def brick_at(n):
        m = jnp.maximum(n, 0)
        return m // (bricks_y * bricks_z), (m // bricks_z) % bricks_y, m % bricks_z

    def stagger(tile, shift):
        sub, _ = iotas()
        for bit in (1, 2, 4):
            turned = pltpu.roll(tile, bit * shift % lanes, 1)
            tile = jnp.where((sub & bit) != 0, turned, tile)
        return tile

    def gather_bricks(source, table, base, count, out):
        sub, lane = iotas()
        keep = ((lane >> 3) & 7) == sub
        pick = (
            lax.broadcasted_iota(jnp.int32, (loads, loads * 8), 1) >> 3
            == lax.broadcasted_iota(jnp.int32, (loads, loads * 8), 0)
        ).astype(F32).astype(BF16)

        def one(r, carry):
            n = table[base + r]
            bx, by, bz = brick_at(n)

            @pl.when(n >= 0)
            def _():
                rows = []
                for l in range(loads):
                    merged = jnp.zeros((8, lanes), F32)
                    for i in range(BE):
                        group = 8 * (i % 2) + i // 2
                        tile = source[l, row(bx * 8 + i, by), :]
                        merged = jnp.where(
                            (lane >> 3) == group,
                            pltpu.roll(tile, (8 * group + lanes - 8 * bz) % lanes, 1),
                            merged,
                        )
                    merged = stagger(merged, 8)
                    columns = []
                    for q in range(4):
                        turned = pltpu.roll(merged, lanes - 8 * q, 1) if q else merged
                        columns.append(jnp.where(keep, turned, 0.0))
                    rows.append(jnp.concatenate(columns, axis=1))
                stacked = jnp.concatenate(rows, axis=0).astype(BF16)
                out[r] = jnp.dot(pick, stacked, preferred_element_type=F32).astype(BF16)

            @pl.when(n < 0)
            def _():
                out[r] = jnp.zeros((loads, cells), BF16)

            return carry

        lax.fori_loop(0, count, one, 0)

    def scatter_bricks(field, table, base, count, images):
        sub, lane = iotas()
        keep = ((lane >> 3) & 7) == sub

        def one(r, carry):
            n = table[base + r]
            bx, by, bz = brick_at(n)
            inside = (lane >> 3) == bz

            @pl.when(n >= 0)
            def _():
                for l in range(loads):
                    merged = jnp.zeros((8, lanes), F32)
                    for q in range(4):
                        spread = jnp.where(
                            keep,
                            jnp.broadcast_to(
                                images[r, pl.ds(l, 1), pl.ds(q * lanes, lanes)], (8, lanes)
                            ),
                            0.0,
                        )
                        merged = merged + (pltpu.roll(spread, 8 * q, 1) if q else spread)
                    merged = stagger(merged, lanes - 8)
                    for i in range(BE):
                        group = 8 * (i % 2) + i // 2
                        turned = pltpu.roll(merged, (8 * bz + lanes - 8 * group) % lanes, 1)
                        at = row(bx * 8 + i, by)
                        field[l, at, :] = jnp.where(inside, turned, field[l, at, :])

            return carry

        lax.fori_loop(0, count, one, 0)

    def pack_depth(read, offsets, source_lane, acc):
        sub, lane = iotas()
        for x in range(X):
            for t in range(T):
                place = offsets + x * T + t
                acc = jnp.where(
                    lane == place,
                    pltpu.roll(read(x, t), (place + lanes - source_lane) % lanes, 1),
                    acc,
                )
        return acc

    def faces(read_tile, read_rows, coords_ref, count, index, outs, pack_index, offset):
        xa, xb, ya, yb, za, zb = outs
        odd = [coords_ref[d] % 2 for d in range(3)]
        for out, low in ((xa, odd[0]), (xb, 1 - odd[0])):
            x = (1 - low) * (X - 1)
            for t in range(T):
                out[index, pl.ds(t * 8, 8), :] = read_tile(x, t)
        for out, low in ((ya, odd[1]), (yb, 1 - odd[1])):
            y = (1 - low) * (Y - 1)
            out[index] = read_rows(y)
        for out, low in ((za, odd[2]), (zb, 1 - odd[2])):
            out[pack_index] = pack_depth(
                read_tile, offset, (1 - low) * (lanes - 1), out[pack_index]
            )

    def unswap(coords_ref, d, a, b, low, high):
        even = coords_ref[d] % 2 == 0
        has_low = coords_ref[d] > 0
        has_high = coords_ref[d] < sizes[d] - 1
        lead = a.shape[0]

        @pl.when(even)
        def _():
            high[...] = a[...]

        @pl.when(jnp.logical_not(even))
        def _():
            low[...] = a[...]

        if sizes[d] > 2:

            @pl.when(even)
            def _():
                low[...] = b[...]

            @pl.when(jnp.logical_not(even))
            def _():
                high[...] = b[...]

        @pl.when(jnp.logical_not(has_low))
        def _():
            low[...] = jnp.zeros(low.shape, F32)

        @pl.when(jnp.logical_not(has_high))
        def _():
            high[...] = jnp.zeros(high.shape, F32)

    def unswap_all(coords_ref, received, halos):
        for d in range(3):
            unswap(coords_ref, d, *received[2 * d : 2 * d + 2], *halos[2 * d : 2 * d + 2])

    def neighbours(read, x, t, first, last, halos, index, pack_index, offset):
        xl, xh, yl, yh, zl, zh = halos
        sub, lane = iotas()
        tile = read(x, t)
        at_t = pl.ds(t * 8, 8)
        x_low = xl[index, at_t, :] if first else read(x - 1, t)
        x_high = xh[index, at_t, :] if last else read(x + 1, t)

        def spread(ref):
            return jnp.broadcast_to(ref[index, pl.ds(x, 1), :], (8, lanes))

        before = spread(yl) if t == 0 else read(x, t - 1)
        after = spread(yh) if t == T - 1 else read(x, t + 1)
        y_low = pltpu.roll(jnp.where(sub == 7, before, tile), 1, 0)
        y_high = pltpu.roll(jnp.where(sub == 0, after, tile), 7, 0)
        place = offset + x * T + t
        z_low = jnp.where(
            lane == 0,
            pltpu.roll(zl[pack_index], (lanes - place) % lanes, 1),
            pltpu.roll(tile, 1, 1),
        )
        z_high = jnp.where(
            lane == lanes - 1,
            pltpu.roll(zh[pack_index], (2 * lanes - 1 - place) % lanes, 1),
            pltpu.roll(tile, lanes - 1, 1),
        )
        return tile, (x_low, x_high, y_low, y_high, z_low, z_high)

    def over_rows(body):
        body(0, True, False)

        def middle(x, carry):
            body(x, False, False)
            return carry

        lax.fori_loop(1, X - 1, middle, 0)
        body(X - 1, False, True)

    def halo_scratch(extra, extra_packs):
        shapes = ((loads + extra, Y, Z), (loads + extra, X, Z), (packs + extra_packs, 8, Z))
        return [pltpu.VMEM(shape, F32) for shape in shapes for _ in range(2)]

    def plain_halo_scratch(count):
        shapes = ((count, Y, Z), (count, X, Z), (1, 8, Z))
        return [pltpu.VMEM(shape, F32) for shape in shapes for _ in range(2)]

    def face_outs(count, pack_count):
        shapes = ((count, Y, Z), (count, X, Z), (pack_count, 8, Z))
        return [(shape, F32, VM) for shape in shapes for _ in range(2)]

    def exchange(payload):
        received = []
        for d, axis in enumerate(AXES):
            n = sizes[d]
            swap_a = [(i, i + 1 if i % 2 == 0 else i - 1) for i in range(n)]
            swap_b = [(i, (i - 1) % n if i % 2 == 0 else (i + 1) % n) for i in range(n)]
            received.append(lax.ppermute(payload[2 * d], axis, swap_a))
            received.append(
                lax.ppermute(payload[2 * d + 1], axis, swap_b) if n > 2 else received[-1]
            )
        return received

    def to_owners(rows, sign):
        parts = []
        for shift in range(1, spans):
            part = rows[(shift - 1) * cap : shift * cap]
            parts.append(
                lax.ppermute(
                    part, "span", [(i, (i + sign * shift) % spans) for i in range(spans)]
                )
            )
        return parts[0] if spans == 2 else jnp.concatenate(parts, axis=0)

    def everyone(partial):
        return lax.all_to_all(partial, AXES, split_axis=0, concat_axis=0, tiled=True)

    def first_kernel(coords_ref, void_ref, owner_ref, load_ref, table_ref, near_ref, far_ref):
        me = coords_ref[0]
        for i in range(slots + 1):
            table_ref[i] = -1
        used = jnp.int32(0)
        for n in range(bricks):
            solid = 1 - void_ref[n]
            relative = jnp.where(solid == 1, (owner_ref[n] + spans - me) % spans, 0)
            shift = relative * bits
            rank = lax.shift_right_logical(used, shift) & ((1 << bits) - 1)
            index = jnp.where(solid == 1, relative * cap + rank, slots)
            table_ref[index] = n
            used = used + lax.shift_left(solid, shift)
        gather_bricks(load_ref, table_ref, cap, remote, far_ref)
        gather_bricks(load_ref, table_ref, 0, cap, near_ref)

    table, near, far = call(
        first_kernel,
        [(coords, SM), (void_f, SM), (owner_f, SM), (load_f, VM)],
        [
            ((slots + 1,), jnp.int32, SM),
            ((cap, loads, cells), BF16, VM),
            ((remote, loads, cells), BF16, VM),
        ],
        name="first",
    )

    step = 2 if cap % 2 == 0 else 1

    def blocks(rows, far_side):
        count = rows.shape[0]

        def kernel(coords_ref, rows_ref, blocks_ref, out_ref):
            for i in range(step):
                out_ref[i] = jnp.dot(
                    rows_ref[i], blocks_ref[i], preferred_element_type=F32
                )

        per = cap // step

        def block_index(r, coords_ref):
            shift = r // per + 1 if far_side else 0
            source = (coords_ref[0] + spans - shift) % spans
            return (source * per + r % per, 0, 0)

        return pl.pallas_call(
            kernel,
            grid_spec=pltpu.PrefetchScalarGridSpec(
                num_scalar_prefetch=1,
                grid=(count // step,),
                in_specs=[
                    pl.BlockSpec((step, loads, cells), lambda r, c: (r, 0, 0)),
                    pl.BlockSpec((step, cells, cells), block_index),
                ],
                out_specs=pl.BlockSpec((step, loads, cells), lambda r, c: (r, 0, 0)),
            ),
            out_shape=jax.ShapeDtypeStruct((count, loads, cells), F32),
            cost_estimate=pl.CostEstimate(
                flops=4000000000, bytes_accessed=count * cells * cells * 2, transcendentals=0
            ),
            name="blocks_far" if far_side else "blocks_near",
        )(coords, rows, precond)

    def precondition(near_rows, far_rows):
        arrived = to_owners(far_rows, 1)
        near_image = blocks(near_rows, False)
        far_image = to_owners(blocks(arrived, True), -1)
        return near_image, far_image

    def near_kernel(with_stiffness):
        def kernel(*refs):
            if with_stiffness:
                table_ref, image_ref, void_ref, phase_ref, field_ref, ks_ref = refs
            else:
                table_ref, image_ref, field_ref = refs
            field_ref[...] = jnp.zeros(field_ref.shape, F32)
            scatter_bricks(field_ref, table_ref, 0, cap, image_ref)
            if with_stiffness:
                sub, lane = iotas()
                for bx in range(bricks_x):
                    for by in range(bricks_y):
                        mask = jnp.zeros((8, lanes), F32)
                        for bz in range(bricks_z):
                            solid = 1 - void_ref[(bx * bricks_y + by) * bricks_z + bz]
                            mask = jnp.where(
                                (lane >> 3) == bz, solid.astype(F32), mask
                            )
                        for i in range(BE):
                            at = row(bx * BE + i, by)
                            p = phase_ref[at, :]
                            stiffness = void_stiffness + (1.0 - void_stiffness) * (p * p * p)
                            ks_ref[at, :] = mask * stiffness

        return kernel

    field_shape = (loads, X * Y, Z)
    plain_shape = (X * Y, Z)

    def far_kernel(extra):
        def kernel(table_ref, coords_ref, image_ref, begun_ref, *refs):
            extras = refs[:extra]
            field_ref = refs[extra]
            outs = refs[extra + 1 :]
            field_ref[...] = begun_ref[...]
            scatter_bricks(field_ref, table_ref, cap, remote, image_ref)
            for out in outs[4:]:
                out[...] = jnp.zeros(out.shape, F32)
            for l in range(loads):
                faces(
                    lambda x, t: field_ref[l, row(x, t), :],
                    lambda y: field_ref[l, pl.ds(y, X, stride=Y), :],
                    coords_ref, loads, l, outs, l // per_pack, (l % per_pack) * tiles,
                )
            for e in range(extra):
                ref = extras[e]
                faces(
                    lambda x, t: ref[row(x, t), :],
                    lambda y: ref[pl.ds(y, X, stride=Y), :],
                    coords_ref, loads, loads + e, outs, packs, e * tiles,
                )

        return kernel

    def to_field(images, extras, with_stiffness):
        near_image, far_image = images
        ins = [(table, SM), (near_image, VM)]
        outs = [(field_shape, F32, VM)]
        if with_stiffness:
            ins += [(void_f, SM), (phase_f, VM)]
            outs += [(plain_shape, F32, VM)]
        made = call(
            near_kernel(with_stiffness), ins, outs, flops=2000000000,
            name="near" + str(len(extras)),
        )
        field = made[0]
        if with_stiffness:
            extras = [made[1]] + extras
        result = call(
            far_kernel(len(extras)),
            [(table, SM), (coords, SM), (far_image, VM), (field, VM)]
            + [(e, VM) for e in extras],
            [(field_shape, F32, VM)] + face_outs(loads + len(extras), packs + 1),
            name="far" + str(len(extras)),
        )
        return result[0], exchange(result[1:]), made[1:]

    z_field, z_halo, (ks,) = to_field(precondition(near, far), [phase_f], True)

    def operate_kernel(
        coords_ref, table_ref, z_ref, load_ref, ks_ref, phase_ref, *refs
    ):
        received = refs[:6]
        q_ref, weight_ref, start_ref, dots_ref, near_ref, far_ref = refs[6:12]
        halos = refs[12:]
        unswap_all(coords_ref, received, halos)
        dots_ref[...] = jnp.zeros(dots_ref.shape, F32)

        def body(x, first, last):
            for t in range(T):
                at = row(x, t)
                ks_tile, ks_near = neighbours(
                    lambda x, t: ks_ref[row(x, t), :],
                    x, t, first, last, halos, loads, packs, 0,
                )
                p, p_near = neighbours(
                    lambda x, t: phase_ref[row(x, t), :],
                    x, t, first, last, halos, loads + 1, packs, tiles,
                )
                around = p_near[0]
                for other in p_near[1:]:
                    around = around + other
                start_ref[at, :] = (
                    p / time_step
                    - 0.5 * p * (1.0 - p) * (1.0 - 2.0 * p)
                    + interface_weight * around
                ) * inverse
                total = jnp.where(ks_tile > 0.0, spring_rate, 0.0)
                weights = []
                for d in range(6):
                    both = jnp.logical_and(ks_tile > 0.0, ks_near[d] > 0.0)
                    weight = jnp.where(both, 0.5 * (ks_tile + ks_near[d]), 0.0)
                    weights.append(weight)
                    weight_ref[d + 1, at, :] = weight
                    total = total + weight
                weight_ref[0, at, :] = total
                for l in range(loads):
                    tile, near_tiles = neighbours(
                        lambda x, t: z_ref[l, row(x, t), :],
                        x, t, first, last, halos, l, l // per_pack, (l % per_pack) * tiles,
                    )
                    image = total * tile
                    for d in range(6):
                        image = image - weights[d] * near_tiles[d]
                    q_ref[l, at, :] = image
                    dots_ref[0, l] += load_ref[l, at, :] * tile
                    dots_ref[1, l] += image * tile

        over_rows(body)
        gather_bricks(q_ref, table_ref, cap, remote, far_ref)
        gather_bricks(q_ref, table_ref, 0, cap, near_ref)

    q_field, weights, start, dots, near, far = call(
        operate_kernel,
        [(coords, SM), (table, SM), (z_field, VM), (load_f, VM), (ks, VM), (phase_f, VM)]
        + [(a, VM) for a in z_halo],
        [
            (field_shape, F32, VM),
            ((7, X * Y, Z), F32, VM),
            (plain_shape, F32, VM),
            ((2, loads, 8, Z), F32, VM),
            ((cap, loads, cells), BF16, VM),
            ((remote, loads, cells), BF16, VM),
        ],
        scratch=halo_scratch(2, 1),
        name="operate",
    )

    w_field, w_halo, _ = to_field(precondition(near, far), [start], False)

    products = 5

    def dots_kernel(
        coords_ref, w_ref, q_ref, load_ref, weight_ref, dots_ref, *refs
    ):
        received = refs[:6]
        out_ref = refs[6]
        more_ref = refs[7]
        halos = refs[8:]
        unswap_all(coords_ref, received, halos)
        more_ref[...] = jnp.zeros(more_ref.shape, F32)

        def body(x, first, last):
            for t in range(T):
                at = row(x, t)
                weights = [weight_ref[d, at, :] for d in range(7)]
                for l in range(loads):
                    tile, near_tiles = neighbours(
                        lambda x, t: w_ref[l, row(x, t), :],
                        x, t, first, last, halos, l, l // per_pack, (l % per_pack) * tiles,
                    )
                    image = weights[0] * tile
                    for d in range(6):
                        image = image - weights[d + 1] * near_tiles[d]
                    more_ref[0, l] += load_ref[l, at, :] * tile
                    more_ref[1, l] += q_ref[l, at, :] * tile
                    more_ref[2, l] += image * tile

        over_rows(body)
        sub, lane = iotas()
        result = jnp.zeros((1, lanes), F32)
        lane1 = lane[:1]
        for k in range(products):
            for l in range(loads):
                part = dots_ref[k, l] if k < 2 else more_ref[k - 2, l]
                value = jnp.sum(jnp.sum(part, axis=0, keepdims=True), axis=1, keepdims=True)
                result = jnp.where(lane1 == k * loads + l, value, result)
        out_ref[...] = jnp.broadcast_to(result, (devices, lanes))

    (partial,) = call(
        dots_kernel,
        [(coords, SM), (w_field, VM), (q_field, VM), (load_f, VM), (weights, VM), (dots, VM)]
        + [(a, VM) for a in w_halo],
        [((devices, lanes), F32, VM)],
        scratch=[pltpu.VMEM((3, loads, 8, Z), F32)] + halo_scratch(1, 1),
        name="dots",
    )
    sums = everyone(partial)

    def solve_kernel(coords_ref, sums_ref, z_ref, w_ref, weight_ref, phase_ref, *refs):
        z_received = refs[:6]
        w_received = refs[6:12]
        x_ref, sens_ref, peak_ref = refs[12:15]
        outs = refs[15:21]
        halos = refs[21:27]
        mixed = refs[27:33]
        sub, lane = iotas()
        total = jnp.sum(sums_ref[...], axis=0, keepdims=True)

        def product(k):
            return pltpu.roll(total, (lanes - k * loads) % lanes, 1)

        total = jnp.broadcast_to(total, (8, lanes))
        bz, zq, bw, qw, ws = [product(k) for k in range(products)]
        alpha = bz / zq
        bz_next = bz - alpha * (bw + zq) + alpha * alpha * qw
        beta = bz_next / bz
        grow = 1.0 + beta
        curvature = grow * grow * zq - 2.0 * grow * alpha * qw + alpha * alpha * ws
        alpha_next = bz_next / curvature
        for_z = alpha + alpha_next * grow
        for_w = -alpha_next * alpha
        c_z = [jnp.broadcast_to(for_z[0:1, l : l + 1], (8, lanes)) for l in range(loads)]
        c_w = [jnp.broadcast_to(for_w[0:1, l : l + 1], (8, lanes)) for l in range(loads)]

        for a, b, out in zip(z_received[:4], w_received[:4], mixed[:4]):
            for l in range(loads):
                for i in range(a.shape[1] // 8):
                    at = pl.ds(i * 8, 8)
                    out[l, at, :] = c_z[l] * a[l, at, :] + c_w[l] * b[l, at, :]
        for a, b, out in zip(z_received[4:], w_received[4:], mixed[4:]):
            for k in range(packs):
                value_z = c_z[k * per_pack]
                value_w = c_w[k * per_pack]
                for i in range(1, per_pack):
                    value_z = jnp.where(lane >= i * tiles, c_z[k * per_pack + i], value_z)
                    value_w = jnp.where(lane >= i * tiles, c_w[k * per_pack + i], value_w)
                out[k] = value_z * a[k] + value_w * b[k]
        unswap_all(coords_ref, mixed, halos)

        def combine(x, carry):
            for t in range(T):
                at = row(x, t)
                for l in range(loads):
                    x_ref[l, at, :] = c_z[l] * z_ref[l, at, :] + c_w[l] * w_ref[l, at, :]
            return carry

        lax.fori_loop(0, X, combine, 0)
        peak_ref[pl.ds(0, 8), :] = jnp.zeros((8, lanes), F32)

        def body(x, first, last):
            for t in range(T):
                at = row(x, t)
                sums_of = [jnp.zeros((8, lanes), F32) for _ in range(6)]
                for l in range(loads):
                    tile, near_tiles = neighbours(
                        lambda x, t: x_ref[l, row(x, t), :],
                        x, t, first, last, halos, l, l // per_pack, (l % per_pack) * tiles,
                    )
                    for d in range(6):
                        gap = tile - near_tiles[d]
                        sums_of[d] = sums_of[d] + gap * gap
                energy = jnp.zeros((8, lanes), F32)
                for d in range(6):
                    energy = energy + jnp.where(
                        weight_ref[d + 1, at, :] > 0.0, sums_of[d], 0.0
                    )
                p = phase_ref[at, :]
                negative = 1.5 * (1.0 - void_stiffness) * (p * p) * energy
                sens_ref[at, :] = -negative
                peak_ref[pl.ds(0, 8), :] = jnp.maximum(peak_ref[pl.ds(0, 8), :], negative)

        over_rows(body)
        peak = jnp.max(
            jnp.max(peak_ref[pl.ds(0, 8), :], axis=0, keepdims=True), axis=1, keepdims=True
        )
        peak_ref[...] = jnp.broadcast_to(peak, (devices, lanes))
        for out in outs[4:]:
            out[...] = jnp.zeros(out.shape, F32)
        faces(
            lambda x, t: sens_ref[row(x, t), :],
            lambda y: sens_ref[pl.ds(y, X, stride=Y), :],
            coords_ref, 0, 0, outs, 0, 0,
        )

    made = call(
        solve_kernel,
        [(coords, SM), (sums, VM), (z_field, VM), (w_field, VM), (weights, VM), (phase_f, VM)]
        + [(a, VM) for a in z_halo]
        + [(a, VM) for a in w_halo],
        [(field_shape, F32, VM), (plain_shape, F32, VM), ((devices, lanes), F32, VM)]
        + face_outs(1, 1),
        scratch=halo_scratch(0, 0) + halo_scratch(0, 0),
        name="solve",
    )
    displacement, sensitivity, peak = made[:3]
    sens_halo = exchange(made[3:])
    peaks = everyone(peak)

    def sweep_kernel(coords_ref, peaks_ref, sens_ref, start_ref, phase_ref, *refs):
        sens_received = refs[:6]
        start_received = refs[6:12]
        out_ref = refs[12]
        once_ref = refs[13]
        halos = refs[14:20]
        mixed = refs[20:26]
        sub, lane = iotas()
        peak = jnp.max(
            jnp.max(peaks_ref[...], axis=0, keepdims=True), axis=1, keepdims=True
        )
        scale = jnp.broadcast_to(1.0 / (peak + epsilon_peak), (8, lanes))
        for s, b, out in zip(sens_received[:4], start_received[:4], mixed[:4]):
            for i in range(out.shape[1] // 8):
                at = pl.ds(i * 8, 8)
                out[0, at, :] = b[loads, at, :] - inverse * (s[0, at, :] * scale)
        for s, b, out in zip(sens_received[4:], start_received[4:], mixed[4:]):
            out[0] = b[packs] - inverse * (s[0] * scale)
        unswap_all(coords_ref, mixed, halos)
        for i in range(tiles):
            at = pl.ds(i * 8, 8)
            once_ref[at, :] = start_ref[at, :] - inverse * (sens_ref[at, :] * scale)

        def body(x, first, last):
            for t in range(T):
                at = row(x, t)
                _, near_tiles = neighbours(
                    lambda x, t: once_ref[row(x, t), :],
                    x, t, first, last, halos, 0, 0, 0,
                )
                around = near_tiles[0]
                for other in near_tiles[1:]:
                    around = around + other
                p = phase_ref[at, :]
                drive = (
                    p / time_step
                    - 0.5 * p * (1.0 - p) * (1.0 - 2.0 * p)
                    - sens_ref[at, :] * scale
                )
                out_ref[at, :] = (drive + interface_weight * around) * inverse

        over_rows(body)

    (phase_next,) = call(
        sweep_kernel,
        [(coords, SM), (peaks, VM), (sensitivity, VM), (start, VM), (phase_f, VM)]
        + [(a, VM) for a in sens_halo]
        + [(a, VM) for a in w_halo],
        [(plain_shape, F32, VM)],
        scratch=[pltpu.VMEM(plain_shape, F32)] + plain_halo_scratch(1) + plain_halo_scratch(1),
        name="sweeps",
    )
    return (
        displacement.reshape(load.shape),
        sensitivity.reshape(phase.shape),
        phase_next.reshape(phase.shape),
    )


def solution(mesh):
    return jax.shard_map(
        local,
        mesh=mesh,
        in_specs=(
            P(None, "span", "height", "depth"),
            P("span", "height", "depth"),
            P("span", "height", "depth"),
            P("span", "height", "depth"),
            P(("span", "height", "depth"), None, None),
        ),
        out_specs=(
            P(None, "span", "height", "depth"),
            P("span", "height", "depth"),
            P("span", "height", "depth"),
        ),
        check_vma=False,
    )
```

```python
import jax
import jax.numpy as jnp
from jax import lax
from jax.experimental import pallas as pl
from jax.experimental.pallas import tpu as pltpu
from jax.sharding import PartitionSpec as P

BE = 8
AXES = ("span", "height", "depth")

void_stiffness = 0.001
spring_rate = 0.05
time_step = 0.5
interface_weight = 0.5
epsilon_peak = 1e-06
inverse = 1.0 / (1.0 / time_step + 6.0 * interface_weight)

F32 = jnp.float32
BF16 = jnp.bfloat16
VM = pl.BlockSpec(memory_space=pltpu.VMEM)
SM = pl.BlockSpec(memory_space=pltpu.SMEM)


HB = pl.BlockSpec(memory_space=pltpu.HBM)


def call(kernel, ins, outs, scratch=(), flops=0, aliases=None, name=None):
    arrays = [
        pltpu.with_memory_space_constraint(array, pltpu.SMEM if spec is SM else pltpu.VMEM)
        for array, spec in ins
    ]
    return pl.pallas_call(
        kernel,
        in_specs=[spec for _, spec in ins],
        out_specs=[spec for _, _, spec in outs],
        out_shape=[
            jax.ShapeDtypeStruct(shape, dtype)
            if spec is HB
            else (pltpu.SMEM if spec is SM else pltpu.VMEM)(shape, dtype)
            for shape, dtype, spec in outs
        ],
        scratch_shapes=list(scratch),
        input_output_aliases=aliases or {},
        cost_estimate=pl.CostEstimate(flops=flops, bytes_accessed=1 << 20, transcendentals=0),
        compiler_params=pltpu.CompilerParams(vmem_limit_bytes=12 << 20),
        name=name,
    )(*arrays)


def slots_fit(bricks, cells):
    return all(n * BE == size for n, size in zip(bricks, cells))


def local(load, phase, void, owner, precond):
    loads, X, Y, Z = load.shape
    bricks_x, bricks_y, bricks_z = void.shape
    bricks = bricks_x * bricks_y * bricks_z
    T = Y // BE
    tiles = X * T
    cells = BE**3
    lanes = Z
    wide = -(-(loads + 2) // 8) * 8
    assert lanes == 128 and BE == 8 and loads == 8 and slots_fit(void.shape, phase.shape)
    sizes = [lax.axis_size(axis) for axis in AXES]
    assert all(size % 2 == 0 for size in sizes)
    spans = sizes[0]
    devices = sizes[0] * sizes[1] * sizes[2]
    slots = precond.shape[0]
    cap = slots // spans
    bits = 32 // spans
    assert cap < (1 << min(bits, 8)) and bits >= 2
    remote = (spans - 1) * cap

    has_b = [size > 2 for size in sizes]
    faces = [(d, b) for d in range(3) for b in range(2) if b == 0 or has_b[d]]
    load_f = load.reshape(loads, X * Y, Z)
    phase_f = phase.reshape(X * Y, Z)

    def iotas():
        return (
            lax.broadcasted_iota(jnp.int32, (8, lanes), 0),
            lax.broadcasted_iota(jnp.int32, (8, lanes), 1),
        )

    def row(x, t):
        start = x * Y + t * 8
        return pl.ds(start if isinstance(start, int) else pl.multiple_of(start, 8), 8)

    def brick_at(n):
        m = jnp.maximum(n, 0)
        return m // (bricks_y * bricks_z), (m // bricks_z) % bricks_y, m % bricks_z

    def spread_of(rows, columns, row_part, column_part):
        r = lax.broadcasted_iota(jnp.int32, (rows, columns), 0)
        c = lax.broadcasted_iota(jnp.int32, (rows, columns), 1)
        same = jnp.logical_and(row_part(r) == column_part(c), (r & 7) == (c & 7))
        return jnp.where(same, 1.0, 0.0).astype(BF16)

    def halves(value):
        high = value.astype(BF16).astype(F32)
        return high, value - high

    def gather_bricks(source, table, base, count, out):
        sub, lane = iotas()
        keep = ((lane >> 3) & 7) == sub
        fold = spread_of(2 * lanes, lanes, lambda r: r >> 7, lambda c: c >> 6)
        pick = jnp.where(
            lax.broadcasted_iota(jnp.int32, (loads, loads * 8), 1) >> 3
            == lax.broadcasted_iota(jnp.int32, (loads, loads * 8), 0),
            1.0,
            0.0,
        ).astype(BF16)

        def one(r, carry):
            n = table[base + r]
            bx, by, bz = brick_at(n)
            inside = (lane >> 3) == bz

            @pl.when(n >= 0)
            def _():
                rows = []
                for q in range(4):
                    for l in range(loads):
                        pair = [
                            jnp.where(inside, source[l, row(bx * 8 + 2 * q + h, by), :], 0.0)
                            for h in range(2)
                        ]
                        rows.append(jnp.concatenate(pair, axis=1))
                stacked = jnp.concatenate(rows, axis=0).astype(BF16)
                folded = jnp.dot(stacked, fold, preferred_element_type=F32)
                columns = []
                for q in range(4):
                    columns.append(
                        jnp.concatenate(
                            [
                                jnp.where(
                                    keep,
                                    folded[(q * loads + l) * 8 : (q * loads + l + 1) * 8],
                                    0.0,
                                )
                                for l in range(loads)
                            ],
                            axis=0,
                        )
                    )
                cells_of = jnp.concatenate(columns, axis=1).astype(BF16)
                out[r] = jnp.dot(pick, cells_of, preferred_element_type=F32).astype(BF16)

            @pl.when(n < 0)
            def _():
                out[r] = jnp.zeros((loads, cells), BF16)

            return carry

        lax.fori_loop(0, count, one, 0)

    def scatter_bricks(field, table, base, count, images, split):
        sub, lane = iotas()
        keep = ((lane >> 3) & 7) == sub
        unfold = spread_of(
            2 * lanes, 2 * lanes, lambda r: (r >> 6) & 1, lambda c: c >> 7
        )

        def one(r, carry):
            n = table[base + r]
            bx, by, bz = brick_at(n)
            inside = (lane >> 3) == bz

            @pl.when(n >= 0)
            def _():
                high, low = halves(images[r])
                split[0] = high
                split[1] = low
                rows = []
                for q in range(4):
                    for l in range(loads):
                        pair = [
                            jnp.where(
                                keep,
                                jnp.broadcast_to(
                                    split[part, pl.ds(l, 1), pl.ds(q * lanes, lanes)],
                                    (8, lanes),
                                ),
                                0.0,
                            )
                            for part in range(2)
                        ]
                        rows.append(jnp.concatenate(pair, axis=1))
                stacked = jnp.concatenate(rows, axis=0).astype(BF16)
                spread = jnp.dot(stacked, unfold, preferred_element_type=F32)
                for q in range(4):
                    for l in range(loads):
                        for h in range(2):
                            at = row(bx * 8 + 2 * q + h, by)
                            tile = spread[
                                (q * loads + l) * 8 : (q * loads + l + 1) * 8,
                                h * lanes : (h + 1) * lanes,
                            ]
                            field[l, at, :] = jnp.where(inside, tile, field[l, at, :])

            return carry

        lax.fori_loop(0, count, one, 0)

    def face_position(coords_ref, d, b, extent):
        high = (coords_ref[d] + b) % 2 == 0
        return jnp.where(high, extent - 1, 0)

    def face_open(coords_ref, d, b):
        if b == 0:
            return jnp.bool_(True)
        return jnp.logical_and(coords_ref[d] > 0, coords_ref[d] < sizes[d] - 1)

    def put_faces(read_tile, read_rows, coords_ref, index, outs):
        for (d, b), out in zip(faces, outs):
            if d == 0:
                x = face_position(coords_ref, d, b, X)
                for t in range(T):
                    out[index, pl.ds(t * 8, 8), :] = read_tile(x, t)
            elif d == 1:
                out[index] = read_rows(face_position(coords_ref, d, b, Y))

    def depth_faces(fields, coords_ref, count):
        rows_i = lax.broadcasted_iota(jnp.int32, (2 * count, lanes), 0)
        lanes_i = lax.broadcasted_iota(jnp.int32, (2 * count, lanes), 1)
        z = [face_position(coords_ref, 2, b, lanes) for b in range(2)]
        total = jnp.zeros((2 * count, X * Y), F32)
        for f, field in enumerate(fields):
            hit = [
                jnp.logical_and(rows_i == b * count + f, lanes_i == z[b]) for b in range(2)
            ]
            pick = jnp.where(jnp.logical_or(*hit), 1.0, 0.0).astype(BF16)
            for part in halves(field()):
                total = total + lax.dot_general(
                    pick,
                    part.astype(BF16),
                    (((1,), (1,)), ((), ())),
                    preferred_element_type=F32,
                )
        return total

    def turned_depth(values):
        return jnp.transpose(jnp.concatenate(halves(values), axis=0)).astype(BF16)

    def spread_depth(turned, coords_ref, rows_of):
        total = turned.shape[1] // 2
        rows_i = lax.broadcasted_iota(jnp.int32, (2 * total, lanes), 0) % total
        lanes_i = lax.broadcasted_iota(jnp.int32, (2 * total, lanes), 1)
        hit = [
            jnp.logical_and(
                rows_i == rows_of[b], lanes_i == face_position(coords_ref, 2, b, lanes)
            )
            for b in range(2)
        ]
        place = jnp.where(jnp.logical_or(*hit), 1.0, 0.0).astype(BF16)
        return jnp.dot(turned, place, preferred_element_type=F32)

    def plain_neighbours(read, x, t):
        sub, lane = iotas()
        tile = read(x, t)
        x_low = read(jnp.maximum(x - 1, 0), t)
        x_high = read(jnp.minimum(x + 1, X - 1), t)
        before = jnp.where(sub == 7, read(x, t - 1), tile) if t > 0 else tile
        after = jnp.where(sub == 0, read(x, t + 1), tile) if t < T - 1 else tile
        return tile, (
            x_low,
            x_high,
            pltpu.roll(before, 1, 0),
            pltpu.roll(after, 7, 0),
            pltpu.roll(tile, 1, 1),
            pltpu.roll(tile, lanes - 1, 1),
        )

    def valid(x, t):
        sub, lane = iotas()
        yes = sub >= 0
        return (
            jnp.logical_and(yes, x > 0),
            jnp.logical_and(yes, x < X - 1),
            sub > 0 if t == 0 else yes,
            sub < 7 if t == T - 1 else yes,
            lane > 0,
            lane < lanes - 1,
        )

    def over_rows(body):
        def one(x, carry):
            body(x)
            return carry

        lax.fori_loop(0, X, one, 0)

    def face_shape(d, count):
        return ((count, Y, Z), (count, X, Z), (-(-count // 8) * 8, X * Y))[d]

    def face_outs(count):
        return [(face_shape(d, count), F32, VM) for d, _ in faces]

    def exchange(payload):
        received = []
        for (d, b), part in zip(faces, payload):
            n = sizes[d]
            swap = [(i, (i + 1 if (i + b) % 2 == 0 else i - 1) % n) for i in range(n)]
            with jax.named_scope("swap" + str(d) + str(b)):
                received.append(lax.ppermute(part, AXES[d], swap))
        return received

    def to_owners(rows, sign):
        parts = []
        for shift in range(1, spans):
            part = rows[(shift - 1) * cap : shift * cap]
            parts.append(
                lax.ppermute(
                    part, "span", [(i, (i + sign * shift) % spans) for i in range(spans)]
                )
            )
        return parts[0] if spans == 2 else jnp.concatenate(parts, axis=0)

    def everyone(partial):
        return lax.all_to_all(partial, AXES, split_axis=0, concat_axis=0, tiled=True)

    field_shape = (loads, X * Y, Z)
    plain_shape = (X * Y, Z)
    face_count = len(faces)

    def first_kernel(
        void_hbm, owner_hbm, load_hbm, phase_hbm, blocks_hbm,
        table_ref, far_ref, load_ref, phase_ref, blocks_ref, coords_ref, void_ref,
        owner_ref, arrived,
    ):
        copies = [
            pltpu.make_async_copy(source, target, arrived.at[i])
            for i, (source, target) in enumerate(
                (
                    (void_hbm, void_ref),
                    (owner_hbm, owner_ref),
                    (load_hbm, load_ref),
                    (phase_hbm, phase_ref),
                    (blocks_hbm, blocks_ref),
                )
            )
        ]
        for copy in copies:
            copy.start()
        for d, axis in enumerate(AXES):
            coords_ref[d] = lax.axis_index(axis)
        me = lax.axis_index("span")
        for i in range(slots + 1):
            table_ref[i] = -1
        copies[0].wait()
        copies[1].wait()
        used = jnp.int32(0)
        for n in range(bricks):
            at = (n // (bricks_y * bricks_z), n // bricks_z % bricks_y, n % bricks_z)
            solid = 1 - void_ref[at]
            relative = jnp.where(solid == 1, (owner_ref[at] + spans - me) % spans, 0)
            shift = relative * bits
            rank = lax.shift_right_logical(used, shift) & ((1 << bits) - 1)
            index = jnp.where(solid == 1, relative * cap + rank, slots)
            table_ref[index] = n
            used = used + lax.shift_left(solid, shift)
        copies[2].wait()
        gather_bricks(load_ref, table_ref, cap, remote, far_ref)
        copies[3].wait()
        copies[4].wait()

    table, far, load_f, phase_f, precond, coords, void = pl.pallas_call(
        first_kernel,
        in_specs=[HB] * 5,
        out_specs=[SM, VM, VM, VM, VM, SM, SM],
        out_shape=[
            pltpu.SMEM((slots + 1,), jnp.int32),
            pltpu.VMEM((remote, loads, cells), BF16),
            pltpu.VMEM(field_shape, F32),
            pltpu.VMEM(plain_shape, F32),
            pltpu.VMEM(precond.shape, BF16),
            pltpu.SMEM((3,), jnp.int32),
            pltpu.SMEM(void.shape, jnp.int32),
        ],
        scratch_shapes=[
            pltpu.SMEM(owner.shape, jnp.int32),
            pltpu.SemaphoreType.DMA((5,)),
        ],
        compiler_params=pltpu.CompilerParams(vmem_limit_bytes=12 << 20),
        name="first",
    )(*[
        pltpu.with_memory_space_constraint(a, pltpu.HBM)
        for a in (void, owner, load_f, phase_f, precond)
    ])

    def near_kernel(
        table_ref, coords_ref, source_ref, blocks_ref, field_ref, rows_ref, image_ref, split
    ):
        field_ref[...] = jnp.zeros(field_ref.shape, F32)
        gather_bricks(source_ref, table_ref, 0, cap, rows_ref)
        for r in range(cap):
            image_ref[r] = jnp.dot(
                rows_ref[r], blocks_ref[coords_ref[0] * cap + r], preferred_element_type=F32
            )
        scatter_bricks(field_ref, table_ref, 0, cap, image_ref, split)

    def near_part(source):
        return call(
            near_kernel,
            [(table, SM), (coords, SM), (source, VM), (precond, VM)],
            [(field_shape, F32, VM)],
            scratch=[
                pltpu.VMEM((cap, loads, cells), BF16),
                pltpu.VMEM((cap, loads, cells), F32),
                pltpu.VMEM((2, loads, cells), F32),
            ],
            flops=8000000000,
            name="near",
        )[0]

    def blocks_kernel(coords_ref, rows_ref, blocks_ref, out_ref):
        for r in range(remote):
            slot = (coords_ref[0] + spans - (r // cap + 1)) % spans * cap + r % cap
            out_ref[r] = jnp.dot(rows_ref[r], blocks_ref[slot], preferred_element_type=F32)

    def far_part(rows):
        (image,) = call(
            blocks_kernel,
            [(coords, SM), (to_owners(rows, 1), VM), (precond, VM)],
            [((remote, loads, cells), F32, VM)],
            name="blocks",
        )
        return to_owners(image, -1)

    def faces_kernel(extra):
        def kernel(table_ref, coords_ref, image_ref, begun_ref, *refs):
            extras = refs[:extra]
            field_ref = refs[extra]
            outs = refs[extra + 1 : extra + 1 + face_count]
            split = refs[extra + 1 + face_count]
            scatter_bricks(field_ref, table_ref, cap, remote, image_ref, split)
            for l in range(loads):
                put_faces(
                    lambda x, t: field_ref[l, row(x, t), :],
                    lambda y: field_ref[l, pl.ds(y, X, stride=Y), :],
                    coords_ref, l, outs,
                )
            for e in range(extra):
                ref = extras[e]
                put_faces(
                    lambda x, t: ref[row(x, t), :],
                    lambda y: ref[pl.ds(y, X, stride=Y), :],
                    coords_ref, loads + e, outs,
                )
            count = outs[-1].shape[0]
            depth = depth_faces(
                [lambda l=l: field_ref[l] for l in range(loads)]
                + [lambda e=e: extras[e][...] for e in range(extra)],
                coords_ref, count,
            )
            for (d, b), out in zip(faces, outs):
                if d == 2:
                    out[...] = depth[b * count : (b + 1) * count]

        return kernel

    def to_field(begun, image, extras):
        result = call(
            faces_kernel(len(extras)),
            [(table, SM), (coords, SM), (image, VM), (begun, VM)]
            + [(e, VM) for e in extras],
            [(field_shape, F32, VM)] + face_outs(loads + len(extras)),
            scratch=[pltpu.VMEM((2, loads, cells), F32)],
            aliases={3: 0},
            name="faces" + str(len(extras)),
        )
        return result[0], result[1:], exchange(result[1:])

    def stiffness_kernel(void_ref, phase_ref, ks_ref):
        sub, lane = iotas()
        for bx in range(bricks_x):
            for by in range(bricks_y):
                mask = jnp.zeros((8, lanes), F32)
                for bz in range(bricks_z):
                    solid = 1 - void_ref[bx, by, bz]
                    mask = jnp.where((lane >> 3) == bz, solid.astype(F32), mask)
                for i in range(BE):
                    at = row(bx * BE + i, by)
                    p = phase_ref[at, :]
                    stiffness = void_stiffness + (1.0 - void_stiffness) * (p * p * p)
                    ks_ref[at, :] = mask * stiffness

    far_image = far_part(far)
    begun = near_part(load_f)
    (ks,) = call(
        stiffness_kernel, [(void, SM), (phase_f, VM)], [(plain_shape, F32, VM)],
        flops=2000000000, name="stiffness",
    )
    z_field, z_sent, z_halo = to_field(begun, far_image, [ks, phase_f])

    def joined(mine, other):
        both = jnp.logical_and(mine > 0.0, other > 0.0)
        return jnp.where(both, 0.5 * (mine + other), 0.0)

    def inner_kernel(z_ref, load_ref, ks_ref, phase_ref, q_ref, weight_ref, start_ref, dots_ref):
        dots_ref[...] = jnp.zeros(dots_ref.shape, F32)

        def body(x):
            for t in range(T):
                at = row(x, t)
                inside = valid(x, t)
                ks_tile, ks_near = plain_neighbours(lambda x, t: ks_ref[row(x, t), :], x, t)
                p, p_near = plain_neighbours(lambda x, t: phase_ref[row(x, t), :], x, t)
                around = jnp.zeros((8, lanes), F32)
                for d in range(6):
                    around = around + jnp.where(inside[d], p_near[d], 0.0)
                start_ref[at, :] = (
                    p / time_step
                    - 0.5 * p * (1.0 - p) * (1.0 - 2.0 * p)
                    + interface_weight * around
                ) * inverse
                total = jnp.where(ks_tile > 0.0, spring_rate, 0.0)
                weights = []
                for d in range(6):
                    weight = jnp.where(inside[d], joined(ks_tile, ks_near[d]), 0.0)
                    weights.append(weight)
                    weight_ref[d, at, :] = weight
                    total = total + weight
                for l in range(loads):
                    tile, near_tiles = plain_neighbours(
                        lambda x, t: z_ref[l, row(x, t), :], x, t
                    )
                    image = total * tile
                    for d in range(6):
                        image = image - weights[d] * near_tiles[d]
                    q_ref[l, at, :] = image
                    dots_ref[0, l] += load_ref[l, at, :] * tile
                    dots_ref[1, l] += image * tile

        over_rows(body)

    q_inner, weights, start_inner, dots = call(
        inner_kernel,
        [(z_field, VM), (load_f, VM), (ks, VM), (phase_f, VM)],
        [
            (field_shape, F32, VM),
            ((6, X * Y, Z), F32, VM),
            (plain_shape, F32, VM),
            ((2, loads, 8, Z), F32, VM),
        ],
        flops=8000000000,
        name="inner",
    )

    def face_weight(coords_ref, d, b, sent, received, at):
        other = jnp.where(face_open(coords_ref, d, b), received[at], 0.0)
        return joined(sent[at], other)

    def row_pieces(d):
        return [pl.ds(i * 8, 8) for i in range((Y if d == 0 else X) // 8)]

    def edges_kernel(coords_ref, table_ref, q_in, start_in, dots_in, *refs):
        sent = refs[:face_count]
        received = refs[face_count : 2 * face_count]
        q_ref, start_ref, dots_ref, far_ref = refs[2 * face_count : 2 * face_count + 4]
        moved = refs[2 * face_count + 4 :]
        scale = interface_weight * inverse
        for (d, b), mine, other, shift in zip(faces, sent, received, moved):
            is_open = face_open(coords_ref, d, b)
            if d < 2:
                for at in row_pieces(d):
                    weight = face_weight(coords_ref, d, b, mine, other, (loads, at))
                    for l in range(loads):
                        tile = mine[l, at, :]
                        change = weight * (tile - other[l, at, :])
                        shift[l, at, :] = change
                        dots_ref[1, l] += tile * change
                    shift[loads, at, :] = jnp.where(
                        is_open, scale * other[loads + 1, at, :], 0.0
                    )
                for l in range(loads + 1):
                    target = q_ref.at[l] if l < loads else start_ref
                    if d == 0:
                        x = face_position(coords_ref, d, b, X)
                        for t in range(T):
                            target[row(x, t), :] += shift[l, pl.ds(t * 8, 8), :]
                    else:
                        y = face_position(coords_ref, d, b, Y)
                        at = pl.ds(y, X, stride=Y)
                        target[at, :] = target[at, :] + shift[l]
            else:
                weight = face_weight(coords_ref, d, b, mine, other, (pl.ds(loads, 1), slice(None)))
                tile = mine[pl.ds(0, loads), :]
                change = weight * (tile - other[pl.ds(0, loads), :])
                shift[pl.ds(0, loads), :] = change
                shift[pl.ds(loads, 8), :] = jnp.zeros((8, X * Y), F32)
                shift[pl.ds(loads, 1), :] = jnp.where(
                    is_open, scale * other[pl.ds(loads + 1, 1), :], 0.0
                )
                product = tile * change
                eight = sum(
                    product[:, i * lanes : (i + 1) * lanes] for i in range(X * Y // lanes)
                )
                sub, lane = iotas()
                for l in range(loads):
                    dots_ref[1, l] += jnp.where(sub == l, eight, 0.0)
        depth = [shift for (d, _), shift in zip(faces, moved) if d == 2]
        turned = turned_depth(jnp.concatenate([ref[...] for ref in depth], axis=0))
        for l in range(loads + 1):
            target = q_ref.at[l] if l < loads else start_ref
            target[...] = target[...] + spread_depth(
                turned, coords_ref, (l, depth[0].shape[0] + l)
            )
        gather_bricks(q_ref, table_ref, cap, remote, far_ref)

    q_field, start, dots, far = call(
        edges_kernel,
        [(coords, SM), (table, SM), (q_inner, VM), (start_inner, VM), (dots, VM)]
        + [(a, VM) for a in z_sent]
        + [(a, VM) for a in z_halo],
        [
            (field_shape, F32, VM),
            (plain_shape, F32, VM),
            ((2, loads, 8, Z), F32, VM),
            ((remote, loads, cells), BF16, VM),
        ],
        scratch=[pltpu.VMEM(face_shape(d, loads + 1), F32) for d, _ in faces],
        aliases={2: 0, 3: 1, 4: 2},
        name="edges",
    )

    far_image = far_part(far)
    w_field, w_sent, w_halo = to_field(near_part(q_field), far_image, [start])

    products = 5

    def more_kernel(w_ref, q_ref, load_ref, weight_ref, ks_ref, more_ref):
        more_ref[...] = jnp.zeros(more_ref.shape, F32)

        def body(x):
            for t in range(T):
                at = row(x, t)
                weights = [weight_ref[d, at, :] for d in (1, 3, 5)]
                spring = jnp.where(ks_ref[at, :] > 0.0, spring_rate, 0.0)
                for l in range(loads):
                    tile, near_tiles = plain_neighbours(
                        lambda x, t: w_ref[l, row(x, t), :], x, t
                    )
                    energy = spring * tile * tile
                    for weight, d in zip(weights, (1, 3, 5)):
                        gap = tile - near_tiles[d]
                        energy = energy + weight * gap * gap
                    more_ref[0, l] += load_ref[l, at, :] * tile
                    more_ref[1, l] += q_ref[l, at, :] * tile
                    more_ref[2, l] += energy

        over_rows(body)

    (more,) = call(
        more_kernel,
        [(w_field, VM), (q_field, VM), (load_f, VM), (weights, VM), (ks, VM)],
        [((3, loads, 8, Z), F32, VM)],
        flops=8000000000,
        name="more",
    )

    def energy_kernel(z_ref, w_ref, ks_ref, energy_ref):
        def body(x):
            for t in range(T):
                at = row(x, t)
                inside = valid(x, t)
                ks_tile, ks_near = plain_neighbours(lambda x, t: ks_ref[row(x, t), :], x, t)
                solid = [
                    jnp.where(
                        jnp.logical_and(inside[d], joined(ks_tile, ks_near[d]) > 0.0), 1.0, 0.0
                    )
                    for d in range(6)
                ]
                for l in range(loads):
                    z, z_near = plain_neighbours(lambda x, t: z_ref[l, row(x, t), :], x, t)
                    w, w_near = plain_neighbours(lambda x, t: w_ref[l, row(x, t), :], x, t)
                    zz = zw = ww = jnp.zeros((8, lanes), F32)
                    for d in range(6):
                        gap_z = solid[d] * (z - z_near[d])
                        gap_w = solid[d] * (w - w_near[d])
                        zz = zz + gap_z * gap_z
                        zw = zw + gap_z * gap_w
                        ww = ww + gap_w * gap_w
                    energy_ref[0, l, at, :] = zz
                    energy_ref[1, l, at, :] = zw
                    energy_ref[2, l, at, :] = ww

        over_rows(body)

    (energies,) = call(
        energy_kernel,
        [(z_field, VM), (w_field, VM), (ks, VM)],
        [((3,) + field_shape, F32, VM)],
        flops=16000000000,
        name="energy",
    )

    def total_kernel(coords_ref, dots_ref, more_in, _, *refs):
        z_mine = refs[:face_count]
        z_other = refs[face_count : 2 * face_count]
        w_mine = refs[2 * face_count : 3 * face_count]
        w_other = refs[3 * face_count : 4 * face_count]
        out_ref, more_ref = refs[4 * face_count : 4 * face_count + 2]
        gaps = refs[4 * face_count + 2 : 5 * face_count + 2]
        starts = refs[5 * face_count + 2 :]
        sub, lane = iotas()
        for (d, b), z_a, z_b, w_a, w_b, gap, begin in zip(
            faces, z_mine, z_other, w_mine, w_other, gaps, starts
        ):
            if d < 2:
                begin[...] = w_b[loads]
                for at in row_pieces(d):
                    weight = face_weight(coords_ref, d, b, z_a, z_b, (loads, at))
                    solid = weight > 0.0
                    for l in range(loads):
                        tile = w_a[l, at, :]
                        between = tile - w_b[l, at, :]
                        more_ref[2, l] += weight * tile * between
                        gap[1, l, at, :] = jnp.where(solid, between, 0.0)
                        gap[0, l, at, :] = jnp.where(
                            solid, z_a[l, at, :] - z_b[l, at, :], 0.0
                        )
            else:
                begin[...] = w_b[pl.ds(loads, 8), :]
                weight = face_weight(coords_ref, d, b, z_a, z_b, (pl.ds(loads, 1), slice(None)))
                solid = weight > 0.0
                tile = w_a[pl.ds(0, loads), :]
                between = tile - w_b[pl.ds(0, loads), :]
                product = weight * tile * between
                gap[1] = jnp.where(solid, between, 0.0)
                gap[0] = jnp.where(
                    solid, z_a[pl.ds(0, loads), :] - z_b[pl.ds(0, loads), :], 0.0
                )
                eight = sum(
                    product[:, i * lanes : (i + 1) * lanes] for i in range(X * Y // lanes)
                )
                for l in range(loads):
                    more_ref[2, l] += jnp.where(sub == l, eight, 0.0)
        result = jnp.zeros((1, lanes), F32)
        lane1 = lane[:1]
        for k in range(products):
            for l in range(loads):
                part = dots_ref[k, l] if k < 2 else more_ref[k - 2, l]
                value = jnp.sum(jnp.sum(part, axis=0, keepdims=True), axis=1, keepdims=True)
                result = jnp.where(lane1 == k * loads + l, value, result)
        out_ref[...] = jnp.broadcast_to(result, (devices, lanes))

    partial, _, *kept = call(
        total_kernel,
        [(coords, SM), (dots, VM), (more, VM), (energies, VM)]
        + [(a, VM) for part in (z_sent, z_halo, w_sent, w_halo) for a in part],
        [((devices, lanes), F32, VM), ((3, loads, 8, Z), F32, VM)]
        + [((2,) + face_shape(d, loads), F32, VM) for d, _ in faces]
        + [((8, X * Y) if d == 2 else face_shape(d, 1)[1:], F32, VM) for d, _ in faces],
        aliases={2: 1},
        name="total",
    )
    gaps, start_halo = kept[:face_count], kept[face_count:]
    sums = everyone(partial)

    def device_beyond(coords_ref, d, b):
        place = [coords_ref[i] for i in range(3)]
        step = jnp.where((place[d] + b) % 2 == 0, 1, -1)
        place[d] = jnp.where(face_open(coords_ref, d, b), place[d] + step, place[d])
        return (place[0] * sizes[1] + place[1]) * sizes[2] + place[2]

    face_rows = max(X, Y)
    message = face_rows + 1

    def solve_kernel(
        coords_ref, sums_ref, energy_ref, phase_ref, z_ref, w_ref, *refs
    ):
        gap_refs = refs[:face_count]
        (sens_ref, out_ref, x_hbm, sens_hbm, x_ref, plain_ref, held_ref, written) = refs[
            face_count:
        ]
        sub, lane = iotas()
        total = jnp.broadcast_to(
            jnp.sum(sums_ref[...], axis=0, keepdims=True), (8, lanes)
        )
        bz, zq, bw, qw, ws = [
            pltpu.roll(total, (lanes - k * loads) % lanes, 1) for k in range(products)
        ]
        alpha = bz / zq
        bz_next = bz - alpha * (bw + zq) + alpha * alpha * qw
        beta = bz_next / bz
        grow = 1.0 + beta
        curvature = grow * grow * zq - 2.0 * grow * alpha * qw + alpha * alpha * ws
        alpha_next = bz_next / curvature
        for_z = alpha + alpha_next * grow
        for_w = -alpha_next * alpha
        c_z = [jnp.broadcast_to(for_z[0:1, l : l + 1], (8, lanes)) for l in range(loads)]
        c_w = [jnp.broadcast_to(for_w[0:1, l : l + 1], (8, lanes)) for l in range(loads)]
        c_zz = [c * c for c in c_z]
        c_zw = [2.0 * a * c for a, c in zip(c_z, c_w)]
        c_ww = [c * c for c in c_w]
        writes = []
        for l in range(loads):

            def mix(i, carry, l=l):
                at = pl.ds(pl.multiple_of(i * 8, 8), 8)
                x_ref[l, at, :] = c_z[l] * z_ref[l, at, :] + c_w[l] * w_ref[l, at, :]
                return carry

            lax.fori_loop(0, tiles, mix, 0, unroll=8)
            writes.append(
                pltpu.make_async_copy(x_ref.at[l], x_hbm.at[l], written.at[l])
            )
            writes[-1].start()

        def body(x):
            for t in range(T):
                at = row(x, t)
                energy = jnp.zeros((8, lanes), F32)
                for l in range(loads):
                    energy = energy + c_zz[l] * energy_ref[0, l, at, :]
                    energy = energy + c_zw[l] * energy_ref[1, l, at, :]
                    energy = energy + c_ww[l] * energy_ref[2, l, at, :]
                plain_ref[at, :] = energy

        over_rows(body)
        held_ref[...] = jnp.zeros(held_ref.shape, F32)
        for (d, b), between in zip(faces, gap_refs):
            if d < 2:
                pieces = []
                for at in row_pieces(d):
                    energy = jnp.zeros((8, lanes), F32)
                    for l in range(loads):
                        gap = c_z[l] * between[0, l, at, :] + c_w[l] * between[1, l, at, :]
                        energy = energy + gap * gap
                    pieces.append(energy)
                if d == 0:
                    x = face_position(coords_ref, d, b, X)
                    for t in range(T):
                        plain_ref[row(x, t), :] += pieces[t]
                else:
                    at = pl.ds(face_position(coords_ref, d, b, Y), X, stride=Y)
                    plain_ref[at, :] = plain_ref[at, :] + jnp.concatenate(pieces, axis=0)
            else:
                by_z = jnp.concatenate([c[0:1, :1] for c in c_z], axis=0)
                by_w = jnp.concatenate([c[0:1, :1] for c in c_w], axis=0)
                gap = by_z * between[0] + by_w * between[1]
                held_ref[pl.ds(b, 1), :] = jnp.sum(gap * gap, axis=0, keepdims=True)
        spread = spread_depth(turned_depth(held_ref[...]), coords_ref, (0, 1))
        energy = plain_ref[...] + spread
        p = phase_ref[...]
        negative = 1.5 * (1.0 - void_stiffness) * (p * p) * energy
        sens_ref[...] = -negative
        writes.append(pltpu.make_async_copy(sens_ref, sens_hbm, written.at[loads]))
        writes[-1].start()
        peak = jnp.max(jnp.max(negative, axis=0, keepdims=True), axis=1, keepdims=True)
        peak = jnp.broadcast_to(peak, (1, lanes))
        high, rest = halves(peak)
        middle, low = halves(rest)
        lane1 = lane[:1]
        tail = jnp.where(lane1 == 0, high, jnp.where(lane1 == 1, middle, low)).astype(BF16)
        for i in range(devices):
            out_ref[i, pl.ds(face_rows, 1), :] = tail
        depth = depth_faces([lambda: sens_ref[...]], coords_ref, 8)
        for d, b in faces:
            @pl.when(face_open(coords_ref, d, b))
            def _(d=d, b=b):
                to = device_beyond(coords_ref, d, b)
                if d == 0:
                    x = face_position(coords_ref, d, b, X)
                    value = sens_ref[pl.ds(pl.multiple_of(x * Y, 8), Y), :]
                elif d == 1:
                    value = sens_ref[
                        pl.ds(face_position(coords_ref, d, b, Y), X, stride=Y), :
                    ]
                else:
                    value = jnp.concatenate(
                        [
                            depth[b * 8 : b * 8 + 1, i * lanes : (i + 1) * lanes]
                            for i in range(X * Y // lanes)
                        ],
                        axis=0,
                    )
                out_ref[to, pl.ds(0, value.shape[0]), :] = value.astype(BF16)
        for write in writes:
            write.wait()

    sens_field, outgoing, displacement, sensitivity = call(
        solve_kernel,
        [
            (coords, SM), (sums, VM), (energies, VM), (phase_f, VM), (z_field, VM),
            (w_field, VM),
        ]
        + [(a, VM) for a in gaps],
        [
            (plain_shape, F32, VM),
            ((devices, message, lanes), BF16, VM),
            (field_shape, F32, HB),
            (plain_shape, F32, HB),
        ],
        scratch=[
            pltpu.VMEM(field_shape, F32),
            pltpu.VMEM(plain_shape, F32),
            pltpu.VMEM((8, X * Y), F32),
            pltpu.SemaphoreType.DMA((loads + 1,)),
        ],
        name="solve",
    )
    incoming = everyone(outgoing)

    def sweep_kernel(coords_ref, in_ref, sens_ref, start_ref, phase_ref, *refs):
        starts = refs[:face_count]
        out_hbm, out_ref, once_ref, held_ref, written = refs[face_count:]
        sub, lane = iotas()
        tails = in_ref[:, pl.ds(face_rows, 1), :].astype(F32)
        tails = tails.reshape(devices, lanes)
        peaks = tails + pltpu.roll(tails, lanes - 1, 1) + pltpu.roll(tails, lanes - 2, 1)
        peak = jnp.max(peaks, axis=0, keepdims=True)[:, :1]
        scale1 = jnp.broadcast_to(1.0 / (peak + epsilon_peak), (1, lanes))
        scale = jnp.broadcast_to(scale1, (8, lanes))
        for i in range(tiles):
            at = pl.ds(i * 8, 8)
            once_ref[at, :] = start_ref[at, :] - inverse * (sens_ref[at, :] * scale)

        def body(x):
            for t in range(T):
                at = row(x, t)
                inside = valid(x, t)
                _, near_tiles = plain_neighbours(lambda x, t: once_ref[row(x, t), :], x, t)
                around = jnp.zeros((8, lanes), F32)
                for d in range(6):
                    around = around + jnp.where(inside[d], near_tiles[d], 0.0)
                p = phase_ref[at, :]
                drive = (
                    p / time_step
                    - 0.5 * p * (1.0 - p) * (1.0 - 2.0 * p)
                    - sens_ref[at, :] * scale
                )
                out_ref[at, :] = (drive + interface_weight * around) * inverse

        over_rows(body)
        held_ref[...] = jnp.zeros(held_ref.shape, F32)
        factor = interface_weight * inverse
        for (d, b), start_b in zip(faces, starts):
            is_open = face_open(coords_ref, d, b)
            source = device_beyond(coords_ref, d, b)
            sent = in_ref[source].astype(F32)
            if d < 2:
                value = start_b[...] - (inverse * scale1) * sent[: (Y if d == 0 else X)]
                value = jnp.where(is_open, factor * value, 0.0)
                if d == 0:
                    x = face_position(coords_ref, d, b, X)
                    at = pl.ds(pl.multiple_of(x * Y, 8), Y)
                else:
                    at = pl.ds(face_position(coords_ref, d, b, Y), X, stride=Y)
                out_ref[at, :] = out_ref[at, :] + value
            else:
                for i in range(X * Y // lanes):
                    at = pl.ds(i * lanes, lanes)
                    value = start_b[pl.ds(0, 1), at] - (inverse * scale1) * sent[i : i + 1]
                    held_ref[pl.ds(b, 1), at] = jnp.where(is_open, factor * value, 0.0)
        out_ref[...] = out_ref[...] + spread_depth(
            turned_depth(held_ref[...]), coords_ref, (0, 1)
        )
        write = pltpu.make_async_copy(out_ref, out_hbm, written)
        write.start()
        write.wait()

    (phase_next,) = call(
        sweep_kernel,
        [(coords, SM), (incoming, VM), (sens_field, VM), (start, VM), (phase_f, VM)]
        + [(a, VM) for a in start_halo],
        [(plain_shape, F32, HB)],
        scratch=[
            pltpu.VMEM(plain_shape, F32),
            pltpu.VMEM(plain_shape, F32),
            pltpu.VMEM((8, X * Y), F32),
            pltpu.SemaphoreType.DMA,
        ],
        name="sweeps",
    )
    return (
        displacement.reshape(load.shape),
        sensitivity.reshape(phase.shape),
        phase_next.reshape(phase.shape),
    )


def solution(mesh):
    return jax.shard_map(
        local,
        mesh=mesh,
        in_specs=(
            P(None, "span", "height", "depth"),
            P("span", "height", "depth"),
            P("span", "height", "depth"),
            P("span", "height", "depth"),
            P(("span", "height", "depth"), None, None),
        ),
        out_specs=(
            P(None, "span", "height", "depth"),
            P("span", "height", "depth"),
            P("span", "height", "depth"),
        ),
        check_vma=False,
    )
```

```python
import jax
import jax.numpy as jnp
from jax import lax
from jax.experimental import pallas as pl
from jax.experimental.pallas import tpu as pltpu
from jax.sharding import PartitionSpec as P


BE = 8
AXES = ("span", "height", "depth")

void_stiffness = 0.001
spring_rate = 0.05
time_step = 0.5
interface_weight = 0.5
epsilon_peak = 1e-06
inverse = 1.0 / (1.0 / time_step + 6.0 * interface_weight)

F32 = jnp.float32
BF16 = jnp.bfloat16
VM = pl.BlockSpec(memory_space=pltpu.VMEM)
SM = pl.BlockSpec(memory_space=pltpu.SMEM)


HB = pl.BlockSpec(memory_space=pltpu.HBM)


def call(kernel, ins, outs, scratch=(), flops=0, aliases=None):
    arrays = [
        pltpu.with_memory_space_constraint(
            array, pltpu.HBM if spec is HB else pltpu.SMEM if spec is SM else pltpu.VMEM
        )
        for array, spec in ins
    ]
    return pl.pallas_call(
        kernel,
        in_specs=[spec for _, spec in ins],
        out_specs=[spec for _, _, spec in outs],
        out_shape=[
            jax.ShapeDtypeStruct(shape, dtype)
            if spec is HB
            else (pltpu.SMEM if spec is SM else pltpu.VMEM)(shape, dtype)
            for shape, dtype, spec in outs
        ],
        scratch_shapes=list(scratch),
        input_output_aliases=aliases or {},
        cost_estimate=pl.CostEstimate(flops=flops, bytes_accessed=1 << 20, transcendentals=0),
        compiler_params=pltpu.CompilerParams(vmem_limit_bytes=12 << 20),
    )(*arrays)


def slots_fit(bricks, cells):
    return all(n * BE == size for n, size in zip(bricks, cells))


def local(load, phase, void, owner, precond):
    loads, X, Y, Z = load.shape
    bricks_x, bricks_y, bricks_z = void.shape
    bricks = bricks_x * bricks_y * bricks_z
    T = Y // BE
    tiles = X * T
    cells = BE**3
    lanes = Z
    assert lanes == 128 and BE == 8 and loads == 8 and slots_fit(void.shape, phase.shape)
    sizes = [lax.axis_size(axis) for axis in AXES]
    assert all(size % 2 == 0 for size in sizes)
    spans = sizes[0]
    devices = sizes[0] * sizes[1] * sizes[2]
    slots = precond.shape[0]
    cap = slots // spans
    bits = 32 // spans
    assert cap < (1 << min(bits, 8)) and bits >= 2
    remote = (spans - 1) * cap

    has_b = [size > 2 for size in sizes]
    faces = [(d, b) for d in range(3) for b in range(2) if b == 0 or has_b[d]]
    load_f = load.reshape(loads, X * Y, Z)
    phase_f = phase.reshape(X * Y, Z)

    def iotas():
        return (
            lax.broadcasted_iota(jnp.int32, (8, lanes), 0),
            lax.broadcasted_iota(jnp.int32, (8, lanes), 1),
        )

    def row(x, t):
        start = x * Y + t * 8
        return pl.ds(start if isinstance(start, int) else pl.multiple_of(start, 8), 8)

    def brick_at(n):
        m = jnp.maximum(n, 0)
        return m // (bricks_y * bricks_z), (m // bricks_z) % bricks_y, m % bricks_z

    def spread_of(rows, columns, row_part, column_part):
        r = lax.broadcasted_iota(jnp.int32, (rows, columns), 0)
        c = lax.broadcasted_iota(jnp.int32, (rows, columns), 1)
        same = jnp.logical_and(row_part(r) == column_part(c), (r & 7) == (c & 7))
        return jnp.where(same, 1.0, 0.0).astype(BF16)

    def halves(value):
        high = value.astype(BF16).astype(F32)
        return high, value - high

    def in_groups(count, one, group=4):
        while count % group:
            group //= 2

        def several(i, carry):
            for j in range(group):
                one(i * group + j)
            return carry

        lax.fori_loop(0, count // group, several, 0)

    def gather_bricks(source, table, base, count, out):
        sub, lane = iotas()
        keep = ((lane >> 3) & 7) == sub
        fold = spread_of(2 * lanes, lanes, lambda r: r >> 7, lambda c: c >> 6)
        pick = jnp.where(
            lax.broadcasted_iota(jnp.int32, (loads, loads * 8), 1) >> 3
            == lax.broadcasted_iota(jnp.int32, (loads, loads * 8), 0),
            1.0,
            0.0,
        ).astype(BF16)

        def one(r):
            n = table[base + r]
            bx, by, bz = brick_at(n)
            inside = (lane >> 3) == jnp.where(n >= 0, bz, -1)
            rows = []
            for q in range(4):
                for l in range(loads):
                    pair = [
                        jnp.where(inside, source[l, row(bx * 8 + 2 * q + h, by), :], 0.0)
                        for h in range(2)
                    ]
                    rows.append(jnp.concatenate(pair, axis=1))
            stacked = jnp.concatenate(rows, axis=0).astype(BF16)
            folded = jnp.dot(stacked, fold, preferred_element_type=F32)
            columns = []
            for q in range(4):
                columns.append(
                    jnp.concatenate(
                        [
                            jnp.where(
                                keep,
                                folded[(q * loads + l) * 8 : (q * loads + l + 1) * 8],
                                0.0,
                            )
                            for l in range(loads)
                        ],
                        axis=0,
                    )
                )
            cells_of = jnp.concatenate(columns, axis=1).astype(BF16)
            out[r] = jnp.dot(pick, cells_of, preferred_element_type=F32).astype(BF16)

        in_groups(count, one)

    def scatter_bricks(field, table, base, count, images, split):
        sub, lane = iotas()
        keep = ((lane >> 3) & 7) == sub
        unfold = spread_of(
            2 * lanes, 2 * lanes, lambda r: (r >> 6) & 1, lambda c: c >> 7
        )

        def one(r):
            n = table[base + r]
            bx, by, bz = brick_at(n)
            inside = (lane >> 3) == jnp.where(n >= 0, bz, -1)
            high, low = halves(images[r])
            split[r, 0] = high
            split[r, 1] = low
            rows = []
            for q in range(4):
                for l in range(loads):
                    pair = [
                        jnp.where(
                            keep,
                            jnp.broadcast_to(
                                split[r, part, pl.ds(l, 1), pl.ds(q * lanes, lanes)],
                                (8, lanes),
                            ),
                            0.0,
                        )
                        for part in range(2)
                    ]
                    rows.append(jnp.concatenate(pair, axis=1))
            stacked = jnp.concatenate(rows, axis=0).astype(BF16)
            spread = jnp.dot(stacked, unfold, preferred_element_type=F32)
            for q in range(4):
                for l in range(loads):
                    for h in range(2):
                        at = row(bx * 8 + 2 * q + h, by)
                        tile = spread[
                            (q * loads + l) * 8 : (q * loads + l + 1) * 8,
                            h * lanes : (h + 1) * lanes,
                        ]
                        field[l, at, :] = jnp.where(inside, tile, field[l, at, :])

        in_groups(count, one)

    def face_position(coords_ref, d, b, extent):
        high = (coords_ref[d] + b) % 2 == 0
        return jnp.where(high, extent - 1, 0)

    def face_open(coords_ref, d, b):
        if b == 0:
            return jnp.bool_(True)
        return jnp.logical_and(coords_ref[d] > 0, coords_ref[d] < sizes[d] - 1)

    def put_faces(read_tile, read_rows, coords_ref, index, outs):
        for (d, b), out in zip(faces, outs):
            if d == 0:
                x = face_position(coords_ref, d, b, X)
                for t in range(T):
                    out[index, pl.ds(t * 8, 8), :] = read_tile(x, t)
            elif d == 1:
                out[index] = read_rows(face_position(coords_ref, d, b, Y))

    def depth_faces(fields, coords_ref, count):
        rows_i = lax.broadcasted_iota(jnp.int32, (2 * count, lanes), 0)
        lanes_i = lax.broadcasted_iota(jnp.int32, (2 * count, lanes), 1)
        z = [face_position(coords_ref, 2, b, lanes) for b in range(2)]
        total = jnp.zeros((2 * count, X * Y), F32)
        for f, field in enumerate(fields):
            hit = [
                jnp.logical_and(rows_i == b * count + f, lanes_i == z[b]) for b in range(2)
            ]
            pick = jnp.where(jnp.logical_or(*hit), 1.0, 0.0).astype(BF16)
            for part in halves(field()):
                total = total + lax.dot_general(
                    pick,
                    part.astype(BF16),
                    (((1,), (1,)), ((), ())),
                    preferred_element_type=F32,
                )
        return total

    def turned_depth(values):
        return jnp.transpose(jnp.concatenate(halves(values), axis=0)).astype(BF16)

    def spread_depth(turned, coords_ref, rows_of):
        total = turned.shape[1] // 2
        rows_i = lax.broadcasted_iota(jnp.int32, (2 * total, lanes), 0) % total
        lanes_i = lax.broadcasted_iota(jnp.int32, (2 * total, lanes), 1)
        hit = [
            jnp.logical_and(
                rows_i == rows_of[b], lanes_i == face_position(coords_ref, 2, b, lanes)
            )
            for b in range(2)
        ]
        place = jnp.where(jnp.logical_or(*hit), 1.0, 0.0).astype(BF16)
        return jnp.dot(turned, place, preferred_element_type=F32)

    def plain_neighbours(read, x, t):
        sub, _ = iotas()
        tile = read(x, t)
        x_low = read(jnp.maximum(x - 1, 0), t)
        x_high = read(jnp.minimum(x + 1, X - 1), t)
        before = jnp.where(sub == 7, read(x, t - 1), tile) if t > 0 else tile
        after = jnp.where(sub == 0, read(x, t + 1), tile) if t < T - 1 else tile
        return tile, (
            x_low,
            x_high,
            pltpu.roll(before, 1, 0),
            pltpu.roll(after, 7, 0),
            pltpu.roll(tile, 1, 1),
            pltpu.roll(tile, lanes - 1, 1),
        )

    def valid(x, t):
        sub, lane = iotas()
        yes = sub >= 0
        return (
            jnp.logical_and(yes, x > 0),
            jnp.logical_and(yes, x < X - 1),
            sub > 0 if t == 0 else yes,
            sub < 7 if t == T - 1 else yes,
            lane > 0,
            lane < lanes - 1,
        )

    def over_rows(body, group=2):
        def several(i, carry):
            for j in range(group):
                body(i * group + j)
            return carry

        lax.fori_loop(0, X // group, several, 0)

    def face_shape(d, count):
        return ((count, Y, Z), (count, X, Z), (-(-count // 8) * 8, X * Y))[d]

    def face_outs(count):
        return [(face_shape(d, count), F32, VM) for d, _ in faces]

    def exchange(payload):
        received = [None] * len(faces)
        for (d, b), part in zip(faces, payload):
            n = sizes[d]
            swap = [(i, (i + 1 if (i + b) % 2 == 0 else i - 1) % n) for i in range(n)]
            received[faces.index((d, b))] = lax.ppermute(part, AXES[d], swap)
        return received

    def to_owners(rows, sign):
        parts = []
        for shift in range(1, spans):
            part = rows[(shift - 1) * cap : shift * cap]
            parts.append(
                lax.ppermute(
                    part, "span", [(i, (i + sign * shift) % spans) for i in range(spans)]
                )
            )
        return parts[0] if spans == 2 else jnp.concatenate(parts, axis=0)

    def everyone(partial):
        return lax.all_to_all(partial, AXES, split_axis=0, concat_axis=0, tiled=True)

    field_shape = (loads, X * Y, Z)
    plain_shape = (X * Y, Z)
    face_count = len(faces)

    def first_kernel(
        void_hbm, owner_hbm, load_hbm, phase_hbm, blocks_hbm,
        table_ref, far_ref, load_ref, phase_ref, blocks_ref, coords_ref, void_ref,
        owner_ref, arrived,
    ):
        me = lax.axis_index("span")
        copies = [
            pltpu.make_async_copy(source, target, arrived.at[i])
            for i, (source, target) in enumerate(
                (
                    (void_hbm, void_ref),
                    (owner_hbm, owner_ref),
                    (load_hbm, load_ref),
                    (phase_hbm, phase_ref),
                    (blocks_hbm.at[pl.ds(me * cap, cap)], blocks_ref),
                )
            )
        ]
        for copy in copies:
            copy.start()
        for d, axis in enumerate(AXES):
            coords_ref[d] = lax.axis_index(axis)
        for i in range(slots + 1):
            table_ref[i] = -1
        copies[0].wait()
        copies[1].wait()
        used = jnp.int32(0)
        for n in range(bricks):
            at = (n // (bricks_y * bricks_z), n // bricks_z % bricks_y, n % bricks_z)
            solid = 1 - void_ref[at]
            relative = jnp.where(solid == 1, (owner_ref[at] + spans - me) % spans, 0)
            shift = relative * bits
            rank = lax.shift_right_logical(used, shift) & ((1 << bits) - 1)
            index = jnp.where(solid == 1, relative * cap + rank, slots)
            table_ref[index] = n
            used = used + lax.shift_left(solid, shift)
        copies[2].wait()
        gather_bricks(load_ref, table_ref, cap, remote, far_ref)
        copies[3].wait()
        copies[4].wait()

    table, far, load_f, phase_f, near_blocks, coords, void = pl.pallas_call(
        first_kernel,
        in_specs=[HB] * 5,
        out_specs=[SM, VM, VM, VM, VM, SM, SM],
        out_shape=[
            pltpu.SMEM((slots + 1,), jnp.int32),
            pltpu.VMEM((remote, loads, cells), BF16),
            pltpu.VMEM(field_shape, F32),
            pltpu.VMEM(plain_shape, F32),
            pltpu.VMEM((cap, cells, cells), BF16),
            pltpu.SMEM((3,), jnp.int32),
            pltpu.SMEM(void.shape, jnp.int32),
        ],
        scratch_shapes=[
            pltpu.SMEM(owner.shape, jnp.int32),
            pltpu.SemaphoreType.DMA((5,)),
        ],
        compiler_params=pltpu.CompilerParams(vmem_limit_bytes=12 << 20),
        name="first",
    )(*[
        pltpu.with_memory_space_constraint(a, pltpu.HBM)
        for a in (void, owner, load_f, phase_f, precond)
    ])

    def near_kernel(bring):
        def kernel(table_ref, coords_ref, source_ref, blocks_ref, *refs):
            copies = []
            if bring:
                hbm, field_ref, far_ref, rows_ref, image_ref, split, arrived = refs
                for shift in range(1, spans):
                    source = (coords_ref[0] + spans - shift) % spans
                    copies.append(
                        pltpu.make_async_copy(
                            hbm.at[pl.ds(source * cap, cap)],
                            far_ref.at[pl.ds((shift - 1) * cap, cap)],
                            arrived.at[shift - 1],
                        )
                    )
                    copies[-1].start()
            else:
                field_ref, rows_ref, image_ref, split = refs
            field_ref[...] = jnp.zeros(field_ref.shape, F32)
            gather_bricks(source_ref, table_ref, 0, cap, rows_ref)
            for r in range(cap):
                image_ref[r] = jnp.dot(
                    rows_ref[r], blocks_ref[r], preferred_element_type=F32
                )
            scatter_bricks(field_ref, table_ref, 0, cap, image_ref, split)
            for copy in copies:
                copy.wait()

        return kernel

    def near_part(source, bring):
        ins = [(table, SM), (coords, SM), (source, VM), (near_blocks, VM)]
        outs = [(field_shape, F32, VM)]
        scratch = [
            pltpu.VMEM((cap, loads, cells), BF16),
            pltpu.VMEM((cap, loads, cells), F32),
            pltpu.VMEM((cap, 2, loads, cells), F32),
        ]
        if bring:
            ins.append((precond, HB))
            outs.append(((remote, cells, cells), BF16, VM))
            scratch.append(pltpu.SemaphoreType.DMA((spans - 1,)))
        return call(near_kernel(bring), ins, outs, scratch=scratch, flops=8000000000)

    def blocks_kernel(rows_ref, blocks_ref, out_ref):
        for r in range(remote):
            out_ref[r] = jnp.dot(rows_ref[r], blocks_ref[r], preferred_element_type=F32)

    def far_part(rows):
        (image,) = call(
            blocks_kernel,
            [(to_owners(rows, 1), VM), (far_blocks, VM)],
            [((remote, loads, cells), F32, VM)],
        )
        return to_owners(image, -1)

    def faces_kernel(extra):
        def kernel(table_ref, coords_ref, image_ref, begun_ref, *refs):
            extras = refs[:extra]
            field_ref = refs[extra]
            outs = refs[extra + 1 : extra + 1 + face_count]
            split = refs[extra + 1 + face_count]
            scatter_bricks(field_ref, table_ref, cap, remote, image_ref, split)
            for l in range(loads):
                put_faces(
                    lambda x, t: field_ref[l, row(x, t), :],
                    lambda y: field_ref[l, pl.ds(y, X, stride=Y), :],
                    coords_ref, l, outs,
                )
            for e in range(extra):
                ref = extras[e]
                put_faces(
                    lambda x, t: ref[row(x, t), :],
                    lambda y: ref[pl.ds(y, X, stride=Y), :],
                    coords_ref, loads + e, outs,
                )
            count = outs[-1].shape[0]
            depth = depth_faces(
                [lambda l=l: field_ref[l] for l in range(loads)]
                + [lambda e=e: extras[e][...] for e in range(extra)],
                coords_ref, count,
            )
            for (d, b), out in zip(faces, outs):
                if d == 2:
                    out[...] = depth[b * count : (b + 1) * count]

        return kernel

    def to_field(begun, image, extras):
        result = call(
            faces_kernel(len(extras)),
            [(table, SM), (coords, SM), (image, VM), (begun, VM)]
            + [(e, VM) for e in extras],
            [(field_shape, F32, VM)] + face_outs(loads + len(extras)),
            scratch=[pltpu.VMEM((remote, 2, loads, cells), F32)],
            aliases={3: 0},
        )
        return result[0], result[1:], exchange(result[1:])

    def stiffness_kernel(void_ref, phase_ref, ks_ref):
        _, lane = iotas()
        for bx in range(bricks_x):
            for by in range(bricks_y):
                mask = jnp.zeros((8, lanes), F32)
                for bz in range(bricks_z):
                    solid = 1 - void_ref[bx, by, bz]
                    mask = jnp.where((lane >> 3) == bz, solid.astype(F32), mask)
                for i in range(BE):
                    at = row(bx * BE + i, by)
                    p = phase_ref[at, :]
                    stiffness = void_stiffness + (1.0 - void_stiffness) * (p * p * p)
                    ks_ref[at, :] = mask * stiffness

    begun, far_blocks = near_part(load_f, True)
    far_image = far_part(far)
    (ks,) = call(
        stiffness_kernel, [(void, SM), (phase_f, VM)], [(plain_shape, F32, VM)],
        flops=2000000000,
    )
    z_field, z_sent, z_halo = to_field(begun, far_image, [ks, phase_f])

    def joined(mine, other):
        both = jnp.logical_and(mine > 0.0, other > 0.0)
        return jnp.where(both, 0.5 * (mine + other), 0.0)

    def inner_kernel(z_ref, load_ref, ks_ref, phase_ref, q_ref, weight_ref, start_ref, dots_ref):
        dots_ref[...] = jnp.zeros(dots_ref.shape, F32)

        def body(x):
            for t in range(T):
                at = row(x, t)
                inside = valid(x, t)
                ks_tile, ks_near = plain_neighbours(lambda x, t: ks_ref[row(x, t), :], x, t)
                p, p_near = plain_neighbours(lambda x, t: phase_ref[row(x, t), :], x, t)
                around = jnp.zeros((8, lanes), F32)
                for d in range(6):
                    around = around + jnp.where(inside[d], p_near[d], 0.0)
                start_ref[at, :] = (
                    p / time_step
                    - 0.5 * p * (1.0 - p) * (1.0 - 2.0 * p)
                    + interface_weight * around
                ) * inverse
                total = jnp.where(ks_tile > 0.0, spring_rate, 0.0)
                weights = []
                for d in range(6):
                    weight = jnp.where(inside[d], joined(ks_tile, ks_near[d]), 0.0)
                    weights.append(weight)
                    weight_ref[d, at, :] = weight
                    total = total + weight
                for l in range(loads):
                    tile, near_tiles = plain_neighbours(
                        lambda x, t: z_ref[l, row(x, t), :], x, t
                    )
                    image = total * tile
                    for d in range(6):
                        image = image - weights[d] * near_tiles[d]
                    q_ref[l, at, :] = image
                    dots_ref[0, l] += load_ref[l, at, :] * tile
                    dots_ref[1, l] += image * tile

        over_rows(body)

    q_inner, weights, start_inner, dots = call(
        inner_kernel,
        [(z_field, VM), (load_f, VM), (ks, VM), (phase_f, VM)],
        [
            (field_shape, F32, VM),
            ((6, X * Y, Z), F32, VM),
            (plain_shape, F32, VM),
            ((2, loads, 8, Z), F32, VM),
        ],
        flops=8000000000,
    )

    def face_weight(coords_ref, d, b, sent, received, at):
        other = jnp.where(face_open(coords_ref, d, b), received[at], 0.0)
        return joined(sent[at], other)

    def row_pieces(d):
        return [pl.ds(i * 8, 8) for i in range((Y if d == 0 else X) // 8)]

    def edges_kernel(coords_ref, table_ref, q_in, start_in, dots_in, *refs):
        sent = refs[:face_count]
        received = refs[face_count : 2 * face_count]
        q_ref, start_ref, dots_ref, far_ref = refs[2 * face_count : 2 * face_count + 4]
        moved = refs[2 * face_count + 4 :]
        scale = interface_weight * inverse
        for (d, b), mine, other, shift in zip(faces, sent, received, moved):
            is_open = face_open(coords_ref, d, b)
            if d < 2:
                for at in row_pieces(d):
                    weight = face_weight(coords_ref, d, b, mine, other, (loads, at))
                    for l in range(loads):
                        tile = mine[l, at, :]
                        change = weight * (tile - other[l, at, :])
                        shift[l, at, :] = change
                        dots_ref[1, l] += tile * change
                    shift[loads, at, :] = jnp.where(
                        is_open, scale * other[loads + 1, at, :], 0.0
                    )
                for l in range(loads + 1):
                    target = q_ref.at[l] if l < loads else start_ref
                    if d == 0:
                        x = face_position(coords_ref, d, b, X)
                        for t in range(T):
                            target[row(x, t), :] += shift[l, pl.ds(t * 8, 8), :]
                    else:
                        y = face_position(coords_ref, d, b, Y)
                        at = pl.ds(y, X, stride=Y)
                        target[at, :] = target[at, :] + shift[l]
            else:
                weight = face_weight(coords_ref, d, b, mine, other, (pl.ds(loads, 1), slice(None)))
                tile = mine[pl.ds(0, loads), :]
                change = weight * (tile - other[pl.ds(0, loads), :])
                shift[pl.ds(0, loads), :] = change
                shift[pl.ds(loads, 8), :] = jnp.zeros((8, X * Y), F32)
                shift[pl.ds(loads, 1), :] = jnp.where(
                    is_open, scale * other[pl.ds(loads + 1, 1), :], 0.0
                )
                product = tile * change
                eight = sum(
                    product[:, i * lanes : (i + 1) * lanes] for i in range(X * Y // lanes)
                )
                sub, _ = iotas()
                for l in range(loads):
                    dots_ref[1, l] += jnp.where(sub == l, eight, 0.0)
        depth = [shift for (d, _), shift in zip(faces, moved) if d == 2]
        turned = turned_depth(jnp.concatenate([ref[...] for ref in depth], axis=0))
        for l in range(loads + 1):
            target = q_ref.at[l] if l < loads else start_ref
            target[...] = target[...] + spread_depth(
                turned, coords_ref, (l, depth[0].shape[0] + l)
            )
        gather_bricks(q_ref, table_ref, cap, remote, far_ref)

    q_field, start, dots, far = call(
        edges_kernel,
        [(coords, SM), (table, SM), (q_inner, VM), (start_inner, VM), (dots, VM)]
        + [(a, VM) for a in z_sent]
        + [(a, VM) for a in z_halo],
        [
            (field_shape, F32, VM),
            (plain_shape, F32, VM),
            ((2, loads, 8, Z), F32, VM),
            ((remote, loads, cells), BF16, VM),
        ],
        scratch=[pltpu.VMEM(face_shape(d, loads + 1), F32) for d, _ in faces],
        aliases={2: 0, 3: 1, 4: 2},
    )

    far_image = far_part(far)
    w_field, w_sent, w_halo = to_field(near_part(q_field, False)[0], far_image, [start])

    products = 5

    def more_kernel(w_ref, q_ref, load_ref, weight_ref, ks_ref, more_ref):
        more_ref[...] = jnp.zeros(more_ref.shape, F32)

        def body(x):
            for t in range(T):
                at = row(x, t)
                weights = [weight_ref[d, at, :] for d in (1, 3, 5)]
                spring = jnp.where(ks_ref[at, :] > 0.0, spring_rate, 0.0)
                for l in range(loads):
                    tile, near_tiles = plain_neighbours(
                        lambda x, t: w_ref[l, row(x, t), :], x, t
                    )
                    energy = spring * tile * tile
                    for weight, d in zip(weights, (1, 3, 5)):
                        gap = tile - near_tiles[d]
                        energy = energy + weight * gap * gap
                    more_ref[0, l] += load_ref[l, at, :] * tile
                    more_ref[1, l] += q_ref[l, at, :] * tile
                    more_ref[2, l] += energy

        over_rows(body)

    (more,) = call(
        more_kernel,
        [(w_field, VM), (q_field, VM), (load_f, VM), (weights, VM), (ks, VM)],
        [((3, loads, 8, Z), F32, VM)],
        flops=8000000000,
    )

    def total_kernel(coords_ref, dots_ref, more_in, *refs):
        z_mine = refs[:face_count]
        z_other = refs[face_count : 2 * face_count]
        w_mine = refs[2 * face_count : 3 * face_count]
        w_other = refs[3 * face_count : 4 * face_count]
        out_ref, more_ref = refs[4 * face_count : 4 * face_count + 2]
        gaps = refs[4 * face_count + 2 : 5 * face_count + 2]
        starts = refs[5 * face_count + 2 :]
        sub, lane = iotas()
        for (d, b), z_a, z_b, w_a, w_b, gap, begin in zip(
            faces, z_mine, z_other, w_mine, w_other, gaps, starts
        ):
            if d < 2:
                begin[...] = w_b[loads]
                for at in row_pieces(d):
                    weight = face_weight(coords_ref, d, b, z_a, z_b, (loads, at))
                    solid = weight > 0.0
                    for l in range(loads):
                        tile = w_a[l, at, :]
                        between = tile - w_b[l, at, :]
                        more_ref[2, l] += weight * tile * between
                        gap[1, l, at, :] = jnp.where(solid, between, 0.0)
                        gap[0, l, at, :] = jnp.where(
                            solid, z_a[l, at, :] - z_b[l, at, :], 0.0
                        )
            else:
                begin[...] = w_b[pl.ds(loads, 8), :]
                weight = face_weight(coords_ref, d, b, z_a, z_b, (pl.ds(loads, 1), slice(None)))
                solid = weight > 0.0
                tile = w_a[pl.ds(0, loads), :]
                between = tile - w_b[pl.ds(0, loads), :]
                product = weight * tile * between
                gap[1] = jnp.where(solid, between, 0.0)
                gap[0] = jnp.where(
                    solid, z_a[pl.ds(0, loads), :] - z_b[pl.ds(0, loads), :], 0.0
                )
                eight = sum(
                    product[:, i * lanes : (i + 1) * lanes] for i in range(X * Y // lanes)
                )
                for l in range(loads):
                    more_ref[2, l] += jnp.where(sub == l, eight, 0.0)
        result = jnp.zeros((1, lanes), F32)
        lane1 = lane[:1]
        for k in range(products):
            for l in range(loads):
                part = dots_ref[k, l] if k < 2 else more_ref[k - 2, l]
                value = jnp.sum(jnp.sum(part, axis=0, keepdims=True), axis=1, keepdims=True)
                result = jnp.where(lane1 == k * loads + l, value, result)
        out_ref[...] = jnp.broadcast_to(result, (devices, lanes))

    partial, _, *kept = call(
        total_kernel,
        [(coords, SM), (dots, VM), (more, VM)]
        + [(a, VM) for part in (z_sent, z_halo, w_sent, w_halo) for a in part],
        [((devices, lanes), F32, VM), ((3, loads, 8, Z), F32, VM)]
        + [((2,) + face_shape(d, loads), F32, VM) for d, _ in faces]
        + [((8, X * Y) if d == 2 else face_shape(d, 1)[1:], F32, VM) for d, _ in faces],
        aliases={2: 1},
    )
    gaps, start_halo = kept[:face_count], kept[face_count:]
    sums = everyone(partial)

    def device_beyond(coords_ref, d, b):
        place = [coords_ref[i] for i in range(3)]
        step = jnp.where((place[d] + b) % 2 == 0, 1, -1)
        place[d] = jnp.where(face_open(coords_ref, d, b), place[d] + step, place[d])
        return (place[0] * sizes[1] + place[1]) * sizes[2] + place[2]

    face_rows = max(X, Y)
    message = face_rows + 1

    def solve_kernel(
        coords_ref, sums_ref, ks_ref, phase_ref, z_ref, w_ref, *refs
    ):
        gap_refs = refs[:face_count]
        sens_ref, out_ref, x_hbm, x_ref, plain_ref, held_ref, written = refs[face_count:]
        _, lane = iotas()
        total = jnp.broadcast_to(
            jnp.sum(sums_ref[...], axis=0, keepdims=True), (8, lanes)
        )
        bz, zq, bw, qw, ws = [
            pltpu.roll(total, (lanes - k * loads) % lanes, 1) for k in range(products)
        ]
        alpha = bz / zq
        bz_next = bz - alpha * (bw + zq) + alpha * alpha * qw
        beta = bz_next / bz
        grow = 1.0 + beta
        curvature = grow * grow * zq - 2.0 * grow * alpha * qw + alpha * alpha * ws
        alpha_next = bz_next / curvature
        for_z = alpha + alpha_next * grow
        for_w = -alpha_next * alpha
        c_z = [jnp.broadcast_to(for_z[0:1, l : l + 1], (8, lanes)) for l in range(loads)]
        c_w = [jnp.broadcast_to(for_w[0:1, l : l + 1], (8, lanes)) for l in range(loads)]
        writes = []
        for l in range(loads):
            for i in range(tiles):
                at = pl.ds(i * 8, 8)
                x_ref[l, at, :] = c_z[l] * z_ref[l, at, :] + c_w[l] * w_ref[l, at, :]
            writes.append(
                pltpu.make_async_copy(x_ref.at[l], x_hbm.at[l], written.at[l])
            )
            writes[-1].start()

        def body(x):
            for t in range(T):
                at = row(x, t)
                inside = valid(x, t)
                ks_tile, ks_near = plain_neighbours(lambda x, t: ks_ref[row(x, t), :], x, t)
                gaps_of = [jnp.zeros((8, lanes), F32) for _ in range(6)]
                for l in range(loads):
                    tile, near_tiles = plain_neighbours(
                        lambda x, t: x_ref[l, row(x, t), :], x, t
                    )
                    for d in range(6):
                        gap = tile - near_tiles[d]
                        gaps_of[d] = gaps_of[d] + gap * gap
                energy = jnp.zeros((8, lanes), F32)
                for d in range(6):
                    solid = jnp.logical_and(inside[d], joined(ks_tile, ks_near[d]) > 0.0)
                    energy = energy + jnp.where(solid, gaps_of[d], 0.0)
                plain_ref[at, :] = energy

        over_rows(body)
        held_ref[...] = jnp.zeros(held_ref.shape, F32)
        for (d, b), between in zip(faces, gap_refs):
            if d < 2:
                pieces = []
                for at in row_pieces(d):
                    energy = jnp.zeros((8, lanes), F32)
                    for l in range(loads):
                        gap = c_z[l] * between[0, l, at, :] + c_w[l] * between[1, l, at, :]
                        energy = energy + gap * gap
                    pieces.append(energy)
                if d == 0:
                    x = face_position(coords_ref, d, b, X)
                    for t in range(T):
                        plain_ref[row(x, t), :] += pieces[t]
                else:
                    at = pl.ds(face_position(coords_ref, d, b, Y), X, stride=Y)
                    plain_ref[at, :] = plain_ref[at, :] + jnp.concatenate(pieces, axis=0)
            else:
                by_z = jnp.concatenate([c[0:1, :1] for c in c_z], axis=0)
                by_w = jnp.concatenate([c[0:1, :1] for c in c_w], axis=0)
                gap = by_z * between[0] + by_w * between[1]
                held_ref[pl.ds(b, 1), :] = jnp.sum(gap * gap, axis=0, keepdims=True)
        spread = spread_depth(turned_depth(held_ref[...]), coords_ref, (0, 1))
        energy = plain_ref[...] + spread
        p = phase_ref[...]
        negative = 1.5 * (1.0 - void_stiffness) * (p * p) * energy
        sens_ref[...] = -negative
        peak = jnp.max(jnp.max(negative, axis=0, keepdims=True), axis=1, keepdims=True)
        peak = jnp.broadcast_to(peak, (1, lanes))
        high, rest = halves(peak)
        middle, low = halves(rest)
        lane1 = lane[:1]
        tail = jnp.where(lane1 == 0, high, jnp.where(lane1 == 1, middle, low)).astype(BF16)
        for i in range(devices):
            out_ref[i, pl.ds(face_rows, 1), :] = tail
        depth = depth_faces([lambda: sens_ref[...]], coords_ref, 8)
        for d, b in faces:
            @pl.when(face_open(coords_ref, d, b))
            def _(d=d, b=b):
                to = device_beyond(coords_ref, d, b)
                if d == 0:
                    x = face_position(coords_ref, d, b, X)
                    value = sens_ref[pl.ds(pl.multiple_of(x * Y, 8), Y), :]
                elif d == 1:
                    value = sens_ref[
                        pl.ds(face_position(coords_ref, d, b, Y), X, stride=Y), :
                    ]
                else:
                    value = jnp.concatenate(
                        [
                            depth[b * 8 : b * 8 + 1, i * lanes : (i + 1) * lanes]
                            for i in range(X * Y // lanes)
                        ],
                        axis=0,
                    )
                out_ref[to, pl.ds(0, value.shape[0]), :] = value.astype(BF16)
        for write in writes:
            write.wait()

    sens_field, outgoing, displacement = call(
        solve_kernel,
        [
            (coords, SM), (sums, VM), (ks, VM), (phase_f, VM), (z_field, VM),
            (w_field, VM),
        ]
        + [(a, VM) for a in gaps],
        [
            (plain_shape, F32, VM),
            ((devices, message, lanes), BF16, VM),
            (field_shape, F32, HB),
        ],
        scratch=[
            pltpu.VMEM(field_shape, F32),
            pltpu.VMEM(plain_shape, F32),
            pltpu.VMEM((8, X * Y), F32),
            pltpu.SemaphoreType.DMA((loads,)),
        ],
    )
    incoming = everyone(outgoing)

    def sweep_kernel(coords_ref, in_ref, sens_ref, start_ref, phase_ref, *refs):
        starts = refs[:face_count]
        out_hbm, sens_hbm, out_ref, once_ref, held_ref, written = refs[face_count:]
        writes = [pltpu.make_async_copy(sens_ref, sens_hbm, written.at[2])]
        writes[0].start()
        sub, lane = iotas()
        tails = in_ref[:, pl.ds(face_rows, 1), :].astype(F32)
        tails = tails.reshape(devices, lanes)
        peaks = tails + pltpu.roll(tails, lanes - 1, 1) + pltpu.roll(tails, lanes - 2, 1)
        peak = jnp.max(peaks, axis=0, keepdims=True)[:, :1]
        scale1 = jnp.broadcast_to(1.0 / (peak + epsilon_peak), (1, lanes))
        scale = jnp.broadcast_to(scale1, (8, lanes))
        for i in range(tiles):
            at = pl.ds(i * 8, 8)
            once_ref[at, :] = start_ref[at, :] - inverse * (sens_ref[at, :] * scale)

        held_ref[...] = jnp.zeros(held_ref.shape, F32)
        factor = interface_weight * inverse
        edges = []
        for (d, b), start_b in zip(faces, starts):
            is_open = face_open(coords_ref, d, b)
            source = device_beyond(coords_ref, d, b)
            sent = in_ref[source].astype(F32)
            if d < 2:
                value = start_b[...] - (inverse * scale1) * sent[: (Y if d == 0 else X)]
                value = jnp.where(is_open, factor * value, 0.0)
                if d == 0:
                    x = face_position(coords_ref, d, b, X)
                    at = pl.ds(pl.multiple_of(x * Y, 8), Y)
                else:
                    at = pl.ds(face_position(coords_ref, d, b, Y), X, stride=Y)
                edges.append((at, value))
            else:
                for i in range(X * Y // lanes):
                    at = pl.ds(i * lanes, lanes)
                    value = start_b[pl.ds(0, 1), at] - (inverse * scale1) * sent[i : i + 1]
                    held_ref[pl.ds(b, 1), at] = jnp.where(is_open, factor * value, 0.0)
        out_ref[...] = spread_depth(turned_depth(held_ref[...]), coords_ref, (0, 1))
        for at, value in edges:
            out_ref[at, :] = out_ref[at, :] + value

        def body(x):
            for t in range(T):
                at = row(x, t)
                inside = valid(x, t)
                _, near_tiles = plain_neighbours(lambda x, t: once_ref[row(x, t), :], x, t)
                around = jnp.zeros((8, lanes), F32)
                for d in range(6):
                    around = around + jnp.where(inside[d], near_tiles[d], 0.0)
                p = phase_ref[at, :]
                drive = (
                    p / time_step
                    - 0.5 * p * (1.0 - p) * (1.0 - 2.0 * p)
                    - sens_ref[at, :] * scale
                )
                out_ref[at, :] += (drive + interface_weight * around) * inverse

        half = X // 2
        for part in range(2):
            for x in range(part * half, (part + 1) * half):
                body(x)
            at = pl.ds(part * half * Y, half * Y)
            writes.append(
                pltpu.make_async_copy(out_ref.at[at], out_hbm.at[at], written.at[part])
            )
            writes[-1].start()
        for write in writes:
            write.wait()

    phase_next, sensitivity = call(
        sweep_kernel,
        [(coords, SM), (incoming, VM), (sens_field, VM), (start, VM), (phase_f, VM)]
        + [(a, VM) for a in start_halo],
        [(plain_shape, F32, HB), (plain_shape, F32, HB)],
        scratch=[
            pltpu.VMEM(plain_shape, F32),
            pltpu.VMEM(plain_shape, F32),
            pltpu.VMEM((8, X * Y), F32),
            pltpu.SemaphoreType.DMA((3,)),
        ],
    )
    return (
        displacement.reshape(load.shape),
        sensitivity.reshape(phase.shape),
        phase_next.reshape(phase.shape),
    )


def solution(mesh):
    return program(mesh)


def program(mesh):
    return jax.shard_map(
        local,
        mesh=mesh,
        in_specs=(
            P(None, "span", "height", "depth"),
            P("span", "height", "depth"),
            P("span", "height", "depth"),
            P("span", "height", "depth"),
            P(("span", "height", "depth"), None, None),
        ),
        out_specs=(
            P(None, "span", "height", "depth"),
            P("span", "height", "depth"),
            P("span", "height", "depth"),
        ),
        check_vma=False,
    )
```

```python
import jax
import jax.numpy as jnp
from jax import lax
from jax.experimental import pallas as pl
from jax.experimental.pallas import tpu as pltpu
from jax.sharding import PartitionSpec as P


BE = 8
AXES = ("span", "height", "depth")

void_stiffness = 0.001
spring_rate = 0.05
time_step = 0.5
interface_weight = 0.5
epsilon_peak = 1e-06
inverse = 1.0 / (1.0 / time_step + 6.0 * interface_weight)

F32 = jnp.float32
BF16 = jnp.bfloat16
VM = pl.BlockSpec(memory_space=pltpu.VMEM)
SM = pl.BlockSpec(memory_space=pltpu.SMEM)


HB = pl.BlockSpec(memory_space=pltpu.HBM)


def call(kernel, ins, outs, scratch=(), flops=0, aliases=None):
    arrays = [
        pltpu.with_memory_space_constraint(
            array, pltpu.HBM if spec is HB else pltpu.SMEM if spec is SM else pltpu.VMEM
        )
        for array, spec in ins
    ]
    return pl.pallas_call(
        kernel,
        in_specs=[spec for _, spec in ins],
        out_specs=[spec for _, _, spec in outs],
        out_shape=[
            jax.ShapeDtypeStruct(shape, dtype)
            if spec is HB
            else (pltpu.SMEM if spec is SM else pltpu.VMEM)(shape, dtype)
            for shape, dtype, spec in outs
        ],
        scratch_shapes=list(scratch),
        input_output_aliases=aliases or {},
        cost_estimate=pl.CostEstimate(flops=flops, bytes_accessed=1 << 20, transcendentals=0),
        compiler_params=pltpu.CompilerParams(vmem_limit_bytes=12 << 20),
    )(*arrays)


def slots_fit(bricks, cells):
    return all(n * BE == size for n, size in zip(bricks, cells))


def local(load, phase, void, owner, precond):
    loads, X, Y, Z = load.shape
    bricks_x, bricks_y, bricks_z = void.shape
    bricks = bricks_x * bricks_y * bricks_z
    T = Y // BE
    tiles = X * T
    cells = BE**3
    lanes = Z
    assert lanes == 128 and BE == 8 and loads == 8 and slots_fit(void.shape, phase.shape)
    sizes = [lax.axis_size(axis) for axis in AXES]
    assert all(size % 2 == 0 for size in sizes)
    spans = sizes[0]
    devices = sizes[0] * sizes[1] * sizes[2]
    slots = precond.shape[0]
    cap = slots // spans
    bits = 32 // spans
    assert cap < (1 << min(bits, 8)) and bits >= 2
    remote = (spans - 1) * cap

    has_b = [size > 2 for size in sizes]
    faces = [(d, b) for d in range(3) for b in range(2) if b == 0 or has_b[d]]
    load_f = load.reshape(loads, X * Y, Z)
    phase_f = phase.reshape(X * Y, Z)

    def iotas():
        return (
            lax.broadcasted_iota(jnp.int32, (8, lanes), 0),
            lax.broadcasted_iota(jnp.int32, (8, lanes), 1),
        )

    def row(x, t):
        start = x * Y + t * 8
        return pl.ds(start if isinstance(start, int) else pl.multiple_of(start, 8), 8)

    def brick_at(n):
        m = jnp.maximum(n, 0)
        return m // (bricks_y * bricks_z), (m // bricks_z) % bricks_y, m % bricks_z

    def spread_of(rows, columns, row_part, column_part):
        r = lax.broadcasted_iota(jnp.int32, (rows, columns), 0)
        c = lax.broadcasted_iota(jnp.int32, (rows, columns), 1)
        same = jnp.logical_and(row_part(r) == column_part(c), (r & 7) == (c & 7))
        return jnp.where(same, 1.0, 0.0).astype(BF16)

    def halves(value):
        high = value.astype(BF16).astype(F32)
        return high, value - high

    def in_groups(count, one, group=4):
        while count % group:
            group //= 2

        def several(i, carry):
            for j in range(group):
                one(i * group + j)
            return carry

        lax.fori_loop(0, count // group, several, 0)

    def gather_bricks(source, table, base, count, out, group=4):
        sub, lane = iotas()
        keep = ((lane >> 3) & 7) == sub
        fold = spread_of(2 * lanes, lanes, lambda r: r >> 7, lambda c: c >> 6)
        pick = jnp.where(
            lax.broadcasted_iota(jnp.int32, (loads, loads * 8), 1) >> 3
            == lax.broadcasted_iota(jnp.int32, (loads, loads * 8), 0),
            1.0,
            0.0,
        ).astype(BF16)

        def one(r):
            n = table[base + r]
            bx, by, bz = brick_at(n)
            inside = (lane >> 3) == jnp.where(n >= 0, bz, -1)
            rows = []
            for q in range(4):
                for l in range(loads):
                    pair = [
                        jnp.where(inside, source[l, row(bx * 8 + 2 * q + h, by), :], 0.0)
                        for h in range(2)
                    ]
                    rows.append(jnp.concatenate(pair, axis=1))
            stacked = jnp.concatenate(rows, axis=0).astype(BF16)
            folded = jnp.dot(stacked, fold, preferred_element_type=F32)
            columns = []
            for q in range(4):
                columns.append(
                    jnp.concatenate(
                        [
                            jnp.where(
                                keep,
                                folded[(q * loads + l) * 8 : (q * loads + l + 1) * 8],
                                0.0,
                            )
                            for l in range(loads)
                        ],
                        axis=0,
                    )
                )
            cells_of = jnp.concatenate(columns, axis=1).astype(BF16)
            out[r] = jnp.dot(pick, cells_of, preferred_element_type=F32).astype(BF16)

        in_groups(count, one, group)

    def scatter_bricks(field, table, base, count, images, split):
        sub, lane = iotas()
        keep = ((lane >> 3) & 7) == sub
        unfold = spread_of(
            2 * lanes, 2 * lanes, lambda r: (r >> 6) & 1, lambda c: c >> 7
        )

        def one(r):
            n = table[base + r]
            bx, by, bz = brick_at(n)
            inside = (lane >> 3) == jnp.where(n >= 0, bz, -1)
            high, low = halves(images[r].astype(F32))
            split[r, 0] = high
            split[r, 1] = low
            rows = []
            for q in range(4):
                for l in range(loads):
                    pair = [
                        jnp.where(
                            keep,
                            jnp.broadcast_to(
                                split[r, part, pl.ds(l, 1), pl.ds(q * lanes, lanes)],
                                (8, lanes),
                            ),
                            0.0,
                        )
                        for part in range(2)
                    ]
                    rows.append(jnp.concatenate(pair, axis=1))
            stacked = jnp.concatenate(rows, axis=0).astype(BF16)
            spread = jnp.dot(stacked, unfold, preferred_element_type=F32)
            for q in range(4):
                for l in range(loads):
                    for h in range(2):
                        at = row(bx * 8 + 2 * q + h, by)
                        tile = spread[
                            (q * loads + l) * 8 : (q * loads + l + 1) * 8,
                            h * lanes : (h + 1) * lanes,
                        ]
                        field[l, at, :] = jnp.where(inside, tile, field[l, at, :])

        in_groups(count, one)

    def face_position(coords_ref, d, b, extent):
        high = (coords_ref[d] + b) % 2 == 0
        return jnp.where(high, extent - 1, 0)

    def face_open(coords_ref, d, b):
        if b == 0:
            return jnp.bool_(True)
        return jnp.logical_and(coords_ref[d] > 0, coords_ref[d] < sizes[d] - 1)

    def put_faces(read_tile, read_rows, coords_ref, index, outs):
        for (d, b), out in zip(faces, outs):
            if d == 0:
                x = face_position(coords_ref, d, b, X)
                for t in range(T):
                    out[index, pl.ds(t * 8, 8), :] = read_tile(x, t)
            elif d == 1:
                out[index] = read_rows(face_position(coords_ref, d, b, Y))

    def depth_faces(fields, coords_ref, count, addends=2):
        rows_i = lax.broadcasted_iota(jnp.int32, (2 * count, lanes), 0)
        lanes_i = lax.broadcasted_iota(jnp.int32, (2 * count, lanes), 1)
        z = [face_position(coords_ref, 2, b, lanes) for b in range(2)]
        total = jnp.zeros((2 * count, X * Y), F32)
        for f, field in enumerate(fields):
            hit = [
                jnp.logical_and(rows_i == b * count + f, lanes_i == z[b]) for b in range(2)
            ]
            pick = jnp.where(jnp.logical_or(*hit), 1.0, 0.0).astype(BF16)
            for part in halves(field())[:addends]:
                total = total + lax.dot_general(
                    pick,
                    part.astype(BF16),
                    (((1,), (1,)), ((), ())),
                    preferred_element_type=F32,
                )
        return total

    def turned_depth(values):
        return jnp.transpose(jnp.concatenate(halves(values), axis=0)).astype(BF16)

    def spread_depth(turned, coords_ref, rows_of):
        total = turned.shape[1] // 2
        rows_i = lax.broadcasted_iota(jnp.int32, (2 * total, lanes), 0) % total
        lanes_i = lax.broadcasted_iota(jnp.int32, (2 * total, lanes), 1)
        hit = [
            jnp.logical_and(
                rows_i == rows_of[b], lanes_i == face_position(coords_ref, 2, b, lanes)
            )
            for b in range(2)
        ]
        place = jnp.where(jnp.logical_or(*hit), 1.0, 0.0).astype(BF16)
        return jnp.dot(turned, place, preferred_element_type=F32)

    def plain_neighbours(read, x, t):
        sub, _ = iotas()
        tile = read(x, t)
        x_low = read(jnp.maximum(x - 1, 0), t)
        x_high = read(jnp.minimum(x + 1, X - 1), t)
        before = jnp.where(sub == 7, read(x, t - 1), tile) if t > 0 else tile
        after = jnp.where(sub == 0, read(x, t + 1), tile) if t < T - 1 else tile
        return tile, (
            x_low,
            x_high,
            pltpu.roll(before, 1, 0),
            pltpu.roll(after, 7, 0),
            pltpu.roll(tile, 1, 1),
            pltpu.roll(tile, lanes - 1, 1),
        )

    def valid(x, t):
        sub, lane = iotas()
        yes = sub >= 0
        return (
            jnp.logical_and(yes, x > 0),
            jnp.logical_and(yes, x < X - 1),
            sub > 0 if t == 0 else yes,
            sub < 7 if t == T - 1 else yes,
            lane > 0,
            lane < lanes - 1,
        )

    def over_rows(body, group=2):
        def several(i, carry):
            for j in range(group):
                body(i * group + j)
            return carry

        lax.fori_loop(0, X // group, several, 0)

    def face_shape(d, count):
        return ((count, Y, Z), (count, X, Z), (-(-count // 8) * 8, X * Y))[d]

    def face_outs(count):
        return [(face_shape(d, count), F32, VM) for d, _ in faces]

    def exchange(payload):
        received = [None] * len(faces)
        for (d, b), part in zip(faces, payload):
            n = sizes[d]
            swap = [(i, (i + 1 if (i + b) % 2 == 0 else i - 1) % n) for i in range(n)]
            received[faces.index((d, b))] = lax.ppermute(part, AXES[d], swap)
        return received

    def to_owners(rows, sign):
        parts = []
        for shift in range(1, spans):
            part = rows[(shift - 1) * cap : shift * cap]
            parts.append(
                lax.ppermute(
                    part, "span", [(i, (i + sign * shift) % spans) for i in range(spans)]
                )
            )
        return parts[0] if spans == 2 else jnp.concatenate(parts, axis=0)

    def everyone(partial):
        return lax.all_to_all(partial, AXES, split_axis=0, concat_axis=0, tiled=True)

    field_shape = (loads, X * Y, Z)
    plain_shape = (X * Y, Z)
    face_count = len(faces)

    def first_kernel(
        void_hbm, owner_hbm, load_hbm, phase_hbm, blocks_hbm,
        table_ref, far_ref, load_ref, phase_ref, blocks_ref, coords_ref, void_ref,
        owner_ref, arrived,
    ):
        me = lax.axis_index("span")
        copies = [
            pltpu.make_async_copy(source, target, arrived.at[i])
            for i, (source, target) in enumerate(
                (
                    (void_hbm, void_ref),
                    (owner_hbm, owner_ref),
                    (load_hbm, load_ref),
                    (phase_hbm, phase_ref),
                    (blocks_hbm.at[pl.ds(me * cap, cap)], blocks_ref),
                )
            )
        ]
        for copy in copies:
            copy.start()
        for d, axis in enumerate(AXES):
            coords_ref[d] = lax.axis_index(axis)
        for i in range(slots + 1):
            table_ref[i] = -1
        copies[0].wait()
        copies[1].wait()
        used = jnp.int32(0)
        for n in range(bricks):
            at = (n // (bricks_y * bricks_z), n // bricks_z % bricks_y, n % bricks_z)
            solid = 1 - void_ref[at]
            relative = jnp.where(solid == 1, (owner_ref[at] + spans - me) % spans, 0)
            shift = relative * bits
            rank = lax.shift_right_logical(used, shift) & ((1 << bits) - 1)
            index = jnp.where(solid == 1, relative * cap + rank, slots)
            table_ref[index] = n
            used = used + lax.shift_left(solid, shift)
        copies[2].wait()
        gather_bricks(load_ref, table_ref, cap, remote, far_ref, group=8)
        copies[3].wait()
        copies[4].wait()

    table, far, load_f, phase_f, near_blocks, coords, void = pl.pallas_call(
        first_kernel,
        in_specs=[HB] * 5,
        out_specs=[SM, VM, VM, VM, VM, SM, SM],
        out_shape=[
            pltpu.SMEM((slots + 1,), jnp.int32),
            pltpu.VMEM((remote, loads, cells), BF16),
            pltpu.VMEM(field_shape, F32),
            pltpu.VMEM(plain_shape, F32),
            pltpu.VMEM((cap, cells, cells), BF16),
            pltpu.SMEM((3,), jnp.int32),
            pltpu.SMEM(void.shape, jnp.int32),
        ],
        scratch_shapes=[
            pltpu.SMEM(owner.shape, jnp.int32),
            pltpu.SemaphoreType.DMA((5,)),
        ],
        compiler_params=pltpu.CompilerParams(vmem_limit_bytes=12 << 20),
        name="first",
    )(*[
        pltpu.with_memory_space_constraint(a, pltpu.HBM)
        for a in (void, owner, load_f, phase_f, precond)
    ])

    def near_kernel(bring):
        def kernel(table_ref, coords_ref, source_ref, blocks_ref, *refs):
            copies = []
            if bring:
                hbm, field_ref, far_ref, rows_ref, image_ref, split, arrived = refs
                for shift in range(1, spans):
                    source = (coords_ref[0] + spans - shift) % spans
                    copies.append(
                        pltpu.make_async_copy(
                            hbm.at[pl.ds(source * cap, cap)],
                            far_ref.at[pl.ds((shift - 1) * cap, cap)],
                            arrived.at[shift - 1],
                        )
                    )
                    copies[-1].start()
            else:
                field_ref, rows_ref, image_ref, split = refs
            field_ref[...] = jnp.zeros(field_ref.shape, F32)
            gather_bricks(source_ref, table_ref, 0, cap, rows_ref)
            for r in range(cap):
                image_ref[r] = jnp.dot(
                    rows_ref[r], blocks_ref[r], preferred_element_type=F32
                )
            scatter_bricks(field_ref, table_ref, 0, cap, image_ref, split)
            for copy in copies:
                copy.wait()

        return kernel

    def near_part(source, bring):
        ins = [(table, SM), (coords, SM), (source, VM), (near_blocks, VM)]
        outs = [(field_shape, F32, VM)]
        scratch = [
            pltpu.VMEM((cap, loads, cells), BF16),
            pltpu.VMEM((cap, loads, cells), F32),
            pltpu.VMEM((cap, 2, loads, cells), F32),
        ]
        if bring:
            ins.append((precond, HB))
            outs.append(((remote, cells, cells), BF16, VM))
            scratch.append(pltpu.SemaphoreType.DMA((spans - 1,)))
        return call(near_kernel(bring), ins, outs, scratch=scratch, flops=8000000000)

    def blocks_kernel(rows_ref, blocks_ref, out_ref):
        for r in range(remote):
            out_ref[r] = jnp.dot(
                rows_ref[r], blocks_ref[r], preferred_element_type=F32
            ).astype(out_ref.dtype)

    def far_part(rows, dtype):
        (image,) = call(
            blocks_kernel,
            [(to_owners(rows, 1), VM), (far_blocks, VM)],
            [((remote, loads, cells), dtype, VM)],
        )
        return to_owners(image, -1)

    def faces_kernel(extra):
        def kernel(table_ref, coords_ref, image_ref, begun_ref, *refs):
            extras = refs[:extra]
            field_ref = refs[extra]
            outs = refs[extra + 1 : extra + 1 + face_count]
            split = refs[extra + 1 + face_count]
            scatter_bricks(field_ref, table_ref, cap, remote, image_ref, split)
            for l in range(loads):
                put_faces(
                    lambda x, t: field_ref[l, row(x, t), :],
                    lambda y: field_ref[l, pl.ds(y, X, stride=Y), :],
                    coords_ref, l, outs,
                )
            for e in range(extra):
                ref = extras[e]
                put_faces(
                    lambda x, t: ref[row(x, t), :],
                    lambda y: ref[pl.ds(y, X, stride=Y), :],
                    coords_ref, loads + e, outs,
                )
            count = outs[-1].shape[0]
            depth = depth_faces(
                [lambda l=l: field_ref[l] for l in range(loads)]
                + [lambda e=e: extras[e][...] for e in range(extra)],
                coords_ref, count, addends=1,
            )
            for (d, b), out in zip(faces, outs):
                if d == 2:
                    out[...] = depth[b * count : (b + 1) * count]

        return kernel

    def to_field(begun, image, extras):
        result = call(
            faces_kernel(len(extras)),
            [(table, SM), (coords, SM), (image, VM), (begun, VM)]
            + [(e, VM) for e in extras],
            [(field_shape, F32, VM)] + face_outs(loads + len(extras)),
            scratch=[pltpu.VMEM((remote, 2, loads, cells), F32)],
            aliases={3: 0},
        )
        return result[0], result[1:], exchange(result[1:])

    def stiffness_kernel(void_ref, phase_ref, ks_ref):
        _, lane = iotas()
        for bx in range(bricks_x):
            for by in range(bricks_y):
                mask = jnp.zeros((8, lanes), F32)
                for bz in range(bricks_z):
                    solid = 1 - void_ref[bx, by, bz]
                    mask = jnp.where((lane >> 3) == bz, solid.astype(F32), mask)
                for i in range(BE):
                    at = row(bx * BE + i, by)
                    p = phase_ref[at, :]
                    stiffness = void_stiffness + (1.0 - void_stiffness) * (p * p * p)
                    ks_ref[at, :] = mask * stiffness

    begun, far_blocks = near_part(load_f, True)
    far_image = far_part(far, F32)
    (ks,) = call(
        stiffness_kernel, [(void, SM), (phase_f, VM)], [(plain_shape, F32, VM)],
        flops=2000000000,
    )
    z_field, z_sent, z_halo = to_field(begun, far_image, [ks, phase_f])

    def joined(mine, other):
        both = jnp.logical_and(mine > 0.0, other > 0.0)
        return jnp.where(both, 0.5 * (mine + other), 0.0)

    def inner_kernel(z_ref, load_ref, ks_ref, phase_ref, q_ref, weight_ref, start_ref, dots_ref):
        dots_ref[...] = jnp.zeros(dots_ref.shape, F32)

        def body(x):
            for t in range(T):
                at = row(x, t)
                inside = valid(x, t)
                ks_tile, ks_near = plain_neighbours(lambda x, t: ks_ref[row(x, t), :], x, t)
                p, p_near = plain_neighbours(lambda x, t: phase_ref[row(x, t), :], x, t)
                around = jnp.zeros((8, lanes), F32)
                for d in range(6):
                    around = around + jnp.where(inside[d], p_near[d], 0.0)
                start_ref[at, :] = (
                    p / time_step
                    - 0.5 * p * (1.0 - p) * (1.0 - 2.0 * p)
                    + interface_weight * around
                ) * inverse
                total = jnp.where(ks_tile > 0.0, spring_rate, 0.0)
                weights = []
                for d in range(6):
                    weight = jnp.where(inside[d], joined(ks_tile, ks_near[d]), 0.0)
                    weights.append(weight)
                    weight_ref[d, at, :] = weight
                    total = total + weight
                for l in range(loads):
                    tile, near_tiles = plain_neighbours(
                        lambda x, t: z_ref[l, row(x, t), :], x, t
                    )
                    image = total * tile
                    for d in range(6):
                        image = image - weights[d] * near_tiles[d]
                    q_ref[l, at, :] = image
                    dots_ref[0, l] += load_ref[l, at, :] * tile
                    dots_ref[1, l] += image * tile

        over_rows(body)

    q_inner, weights, start_inner, dots = call(
        inner_kernel,
        [(z_field, VM), (load_f, VM), (ks, VM), (phase_f, VM)],
        [
            (field_shape, F32, VM),
            ((6, X * Y, Z), F32, VM),
            (plain_shape, F32, VM),
            ((2, loads, 8, Z), F32, VM),
        ],
        flops=8000000000,
    )

    def face_weight(coords_ref, d, b, sent, received, at):
        other = jnp.where(face_open(coords_ref, d, b), received[at], 0.0)
        return joined(sent[at], other)

    def row_pieces(d):
        return [pl.ds(i * 8, 8) for i in range((Y if d == 0 else X) // 8)]

    def edges_kernel(coords_ref, table_ref, q_in, start_in, dots_in, *refs):
        sent = refs[:face_count]
        received = refs[face_count : 2 * face_count]
        q_ref, start_ref, dots_ref, far_ref = refs[2 * face_count : 2 * face_count + 4]
        moved = refs[2 * face_count + 4 :]
        scale = interface_weight * inverse
        for (d, b), mine, other, shift in zip(faces, sent, received, moved):
            is_open = face_open(coords_ref, d, b)
            if d < 2:
                for at in row_pieces(d):
                    weight = face_weight(coords_ref, d, b, mine, other, (loads, at))
                    for l in range(loads):
                        tile = mine[l, at, :]
                        change = weight * (tile - other[l, at, :])
                        shift[l, at, :] = change
                        dots_ref[1, l] += tile * change
                    shift[loads, at, :] = jnp.where(
                        is_open, scale * other[loads + 1, at, :], 0.0
                    )
                for l in range(loads + 1):
                    target = q_ref.at[l] if l < loads else start_ref
                    if d == 0:
                        x = face_position(coords_ref, d, b, X)
                        for t in range(T):
                            target[row(x, t), :] += shift[l, pl.ds(t * 8, 8), :]
                    else:
                        y = face_position(coords_ref, d, b, Y)
                        at = pl.ds(y, X, stride=Y)
                        target[at, :] = target[at, :] + shift[l]
            else:
                weight = face_weight(coords_ref, d, b, mine, other, (pl.ds(loads, 1), slice(None)))
                tile = mine[pl.ds(0, loads), :]
                change = weight * (tile - other[pl.ds(0, loads), :])
                shift[pl.ds(0, loads), :] = change
                shift[pl.ds(loads, 8), :] = jnp.zeros((8, X * Y), F32)
                shift[pl.ds(loads, 1), :] = jnp.where(
                    is_open, scale * other[pl.ds(loads + 1, 1), :], 0.0
                )
                product = tile * change
                eight = sum(
                    product[:, i * lanes : (i + 1) * lanes] for i in range(X * Y // lanes)
                )
                sub, _ = iotas()
                for l in range(loads):
                    dots_ref[1, l] += jnp.where(sub == l, eight, 0.0)
        depth = [shift for (d, _), shift in zip(faces, moved) if d == 2]
        turned = turned_depth(jnp.concatenate([ref[...] for ref in depth], axis=0))
        for l in range(loads + 1):
            target = q_ref.at[l] if l < loads else start_ref
            target[...] = target[...] + spread_depth(
                turned, coords_ref, (l, depth[0].shape[0] + l)
            )
        gather_bricks(q_ref, table_ref, cap, remote, far_ref)

    q_field, start, dots, far = call(
        edges_kernel,
        [(coords, SM), (table, SM), (q_inner, VM), (start_inner, VM), (dots, VM)]
        + [(a, VM) for a in z_sent]
        + [(a, VM) for a in z_halo],
        [
            (field_shape, F32, VM),
            (plain_shape, F32, VM),
            ((2, loads, 8, Z), F32, VM),
            ((remote, loads, cells), BF16, VM),
        ],
        scratch=[pltpu.VMEM(face_shape(d, loads + 1), F32) for d, _ in faces],
        aliases={2: 0, 3: 1, 4: 2},
    )

    far_image = far_part(far, BF16)
    w_field, w_sent, w_halo = to_field(near_part(q_field, False)[0], far_image, [start])

    products = 5

    def more_kernel(w_ref, q_ref, load_ref, weight_ref, ks_ref, more_ref):
        more_ref[...] = jnp.zeros(more_ref.shape, F32)

        def body(x):
            for t in range(T):
                at = row(x, t)
                weights = [weight_ref[d, at, :] for d in (1, 3, 5)]
                spring = jnp.where(ks_ref[at, :] > 0.0, spring_rate, 0.0)
                for l in range(loads):
                    tile, near_tiles = plain_neighbours(
                        lambda x, t: w_ref[l, row(x, t), :], x, t
                    )
                    energy = spring * tile * tile
                    for weight, d in zip(weights, (1, 3, 5)):
                        gap = tile - near_tiles[d]
                        energy = energy + weight * gap * gap
                    more_ref[0, l] += load_ref[l, at, :] * tile
                    more_ref[1, l] += q_ref[l, at, :] * tile
                    more_ref[2, l] += energy

        over_rows(body)

    (more,) = call(
        more_kernel,
        [(w_field, VM), (q_field, VM), (load_f, VM), (weights, VM), (ks, VM)],
        [((3, loads, 8, Z), F32, VM)],
        flops=8000000000,
    )

    def total_kernel(coords_ref, dots_ref, more_in, *refs):
        z_mine = refs[:face_count]
        z_other = refs[face_count : 2 * face_count]
        w_mine = refs[2 * face_count : 3 * face_count]
        w_other = refs[3 * face_count : 4 * face_count]
        out_ref, more_ref = refs[4 * face_count : 4 * face_count + 2]
        gaps = refs[4 * face_count + 2 : 5 * face_count + 2]
        starts = refs[5 * face_count + 2 :]
        sub, lane = iotas()
        for (d, b), z_a, z_b, w_a, w_b, gap, begin in zip(
            faces, z_mine, z_other, w_mine, w_other, gaps, starts
        ):
            if d < 2:
                begin[...] = w_b[loads]
                for at in row_pieces(d):
                    weight = face_weight(coords_ref, d, b, z_a, z_b, (loads, at))
                    solid = weight > 0.0
                    for l in range(loads):
                        tile = w_a[l, at, :]
                        between = tile - w_b[l, at, :]
                        more_ref[2, l] += weight * tile * between
                        gap[1, l, at, :] = jnp.where(solid, between, 0.0)
                        gap[0, l, at, :] = jnp.where(
                            solid, z_a[l, at, :] - z_b[l, at, :], 0.0
                        )
            else:
                begin[...] = w_b[pl.ds(loads, 8), :]
                weight = face_weight(coords_ref, d, b, z_a, z_b, (pl.ds(loads, 1), slice(None)))
                solid = weight > 0.0
                tile = w_a[pl.ds(0, loads), :]
                between = tile - w_b[pl.ds(0, loads), :]
                product = weight * tile * between
                gap[1] = jnp.where(solid, between, 0.0)
                gap[0] = jnp.where(
                    solid, z_a[pl.ds(0, loads), :] - z_b[pl.ds(0, loads), :], 0.0
                )
                eight = sum(
                    product[:, i * lanes : (i + 1) * lanes] for i in range(X * Y // lanes)
                )
                for l in range(loads):
                    more_ref[2, l] += jnp.where(sub == l, eight, 0.0)
        result = jnp.zeros((1, lanes), F32)
        lane1 = lane[:1]
        for k in range(products):
            for l in range(loads):
                part = dots_ref[k, l] if k < 2 else more_ref[k - 2, l]
                value = jnp.sum(jnp.sum(part, axis=0, keepdims=True), axis=1, keepdims=True)
                result = jnp.where(lane1 == k * loads + l, value, result)
        out_ref[...] = jnp.broadcast_to(result, (devices, lanes))

    partial, _, *kept = call(
        total_kernel,
        [(coords, SM), (dots, VM), (more, VM)]
        + [(a, VM) for part in (z_sent, z_halo, w_sent, w_halo) for a in part],
        [((devices, lanes), F32, VM), ((3, loads, 8, Z), F32, VM)]
        + [((2,) + face_shape(d, loads), F32, VM) for d, _ in faces]
        + [((8, X * Y) if d == 2 else face_shape(d, 1)[1:], F32, VM) for d, _ in faces],
        aliases={2: 1},
    )
    gaps, start_halo = kept[:face_count], kept[face_count:]
    sums = everyone(partial)

    def device_beyond(coords_ref, d, b):
        place = [coords_ref[i] for i in range(3)]
        step = jnp.where((place[d] + b) % 2 == 0, 1, -1)
        place[d] = jnp.where(face_open(coords_ref, d, b), place[d] + step, place[d])
        return (place[0] * sizes[1] + place[1]) * sizes[2] + place[2]

    face_rows = max(X, Y)
    message = face_rows + 1

    def solve_kernel(
        coords_ref, sums_ref, ks_ref, phase_ref, z_ref, w_ref, *refs
    ):
        gap_refs = refs[:face_count]
        sens_ref, out_ref, x_hbm, x_ref, plain_ref, link_ref, held_ref, written = refs[
            face_count:
        ]
        sub, lane = iotas()
        total = jnp.broadcast_to(
            jnp.sum(sums_ref[...], axis=0, keepdims=True), (8, lanes)
        )
        bz, zq, bw, qw, ws = [
            pltpu.roll(total, (lanes - k * loads) % lanes, 1) for k in range(products)
        ]
        alpha = bz / zq
        bz_next = bz - alpha * (bw + zq) + alpha * alpha * qw
        beta = bz_next / bz
        grow = 1.0 + beta
        curvature = grow * grow * zq - 2.0 * grow * alpha * qw + alpha * alpha * ws
        alpha_next = bz_next / curvature
        for_z = alpha + alpha_next * grow
        for_w = -alpha_next * alpha
        c_z = [jnp.broadcast_to(for_z[0:1, l : l + 1], (8, lanes)) for l in range(loads)]
        c_w = [jnp.broadcast_to(for_w[0:1, l : l + 1], (8, lanes)) for l in range(loads)]
        writes = []
        for l in range(loads):
            for i in range(tiles):
                at = pl.ds(i * 8, 8)
                x_ref[l, at, :] = c_z[l] * z_ref[l, at, :] + c_w[l] * w_ref[l, at, :]
            writes.append(
                pltpu.make_async_copy(x_ref.at[l], x_hbm.at[l], written.at[l])
            )
            writes[-1].start()

        def body(x):
            for t in range(T):
                at = row(x, t)
                inside = valid(x, t)
                ks_tile, ks_near = plain_neighbours(lambda x, t: ks_ref[row(x, t), :], x, t)
                gaps_of = [jnp.zeros((8, lanes), F32) for _ in range(3)]
                for l in range(loads):
                    tile, near_tiles = plain_neighbours(
                        lambda x, t: x_ref[l, row(x, t), :], x, t
                    )
                    for d in range(3):
                        gap = tile - near_tiles[2 * d + 1]
                        gaps_of[d] = gaps_of[d] + gap * gap
                for d in range(3):
                    n = 2 * d + 1
                    solid = jnp.logical_and(inside[n], joined(ks_tile, ks_near[n]) > 0.0)
                    link_ref[d, at, :] = jnp.where(solid, gaps_of[d], 0.0)

        over_rows(body)
        for x in range(X):
            for t in range(T):
                at = row(x, t)
                along_y = link_ref[1, at, :]
                before = link_ref[1, row(x, t - 1), :] if t > 0 else 0.0
                along_z = link_ref[2, at, :]
                energy = link_ref[0, at, :] + along_y + along_z
                energy = energy + pltpu.roll(jnp.where(sub == 7, before, along_y), 1, 0)
                energy = energy + pltpu.roll(along_z, 1, 1)
                if x > 0:
                    energy = energy + link_ref[0, row(x - 1, t), :]
                plain_ref[at, :] = energy
        held_ref[...] = jnp.zeros(held_ref.shape, F32)
        for (d, b), between in zip(faces, gap_refs):
            if d < 2:
                pieces = []
                for at in row_pieces(d):
                    energy = jnp.zeros((8, lanes), F32)
                    for l in range(loads):
                        gap = c_z[l] * between[0, l, at, :] + c_w[l] * between[1, l, at, :]
                        energy = energy + gap * gap
                    pieces.append(energy)
                if d == 0:
                    x = face_position(coords_ref, d, b, X)
                    for t in range(T):
                        plain_ref[row(x, t), :] += pieces[t]
                else:
                    at = pl.ds(face_position(coords_ref, d, b, Y), X, stride=Y)
                    plain_ref[at, :] = plain_ref[at, :] + jnp.concatenate(pieces, axis=0)
            else:
                by_z = jnp.concatenate([c[0:1, :1] for c in c_z], axis=0)
                by_w = jnp.concatenate([c[0:1, :1] for c in c_w], axis=0)
                gap = by_z * between[0] + by_w * between[1]
                held_ref[pl.ds(b, 1), :] = jnp.sum(gap * gap, axis=0, keepdims=True)
        spread = spread_depth(turned_depth(held_ref[...]), coords_ref, (0, 1))
        energy = plain_ref[...] + spread
        p = phase_ref[...]
        negative = 1.5 * (1.0 - void_stiffness) * (p * p) * energy
        sens_ref[...] = -negative
        peak = jnp.max(jnp.max(negative, axis=0, keepdims=True), axis=1, keepdims=True)
        peak = jnp.broadcast_to(peak, (1, lanes))
        high, rest = halves(peak)
        middle, low = halves(rest)
        lane1 = lane[:1]
        tail = jnp.where(lane1 == 0, high, jnp.where(lane1 == 1, middle, low)).astype(BF16)
        for i in range(devices):
            out_ref[i, pl.ds(face_rows, 1), :] = tail
        depth = depth_faces([lambda: sens_ref[...]], coords_ref, 8, addends=1)
        for d, b in faces:
            @pl.when(face_open(coords_ref, d, b))
            def _(d=d, b=b):
                to = device_beyond(coords_ref, d, b)
                if d == 0:
                    x = face_position(coords_ref, d, b, X)
                    value = sens_ref[pl.ds(pl.multiple_of(x * Y, 8), Y), :]
                elif d == 1:
                    value = sens_ref[
                        pl.ds(face_position(coords_ref, d, b, Y), X, stride=Y), :
                    ]
                else:
                    value = jnp.concatenate(
                        [
                            depth[b * 8 : b * 8 + 1, i * lanes : (i + 1) * lanes]
                            for i in range(X * Y // lanes)
                        ],
                        axis=0,
                    )
                out_ref[to, pl.ds(0, value.shape[0]), :] = value.astype(BF16)
        for write in writes:
            write.wait()

    sens_field, outgoing, displacement = call(
        solve_kernel,
        [
            (coords, SM), (sums, VM), (ks, VM), (phase_f, VM), (z_field, VM),
            (w_field, VM),
        ]
        + [(a, VM) for a in gaps],
        [
            (plain_shape, F32, VM),
            ((devices, message, lanes), BF16, VM),
            (field_shape, F32, HB),
        ],
        scratch=[
            pltpu.VMEM(field_shape, F32),
            pltpu.VMEM(plain_shape, F32),
            pltpu.VMEM((3,) + plain_shape, F32),
            pltpu.VMEM((8, X * Y), F32),
            pltpu.SemaphoreType.DMA((loads,)),
        ],
    )
    incoming = everyone(outgoing)

    def sweep_kernel(coords_ref, in_ref, sens_ref, start_ref, phase_ref, *refs):
        starts = refs[:face_count]
        out_hbm, sens_hbm, out_ref, once_ref, held_ref, written = refs[face_count:]
        writes = [pltpu.make_async_copy(sens_ref, sens_hbm, written.at[2])]
        writes[0].start()
        sub, lane = iotas()
        tails = in_ref[:, pl.ds(face_rows, 1), :].astype(F32)
        tails = tails.reshape(devices, lanes)
        peaks = tails + pltpu.roll(tails, lanes - 1, 1) + pltpu.roll(tails, lanes - 2, 1)
        peak = jnp.max(peaks, axis=0, keepdims=True)[:, :1]
        scale1 = jnp.broadcast_to(1.0 / (peak + epsilon_peak), (1, lanes))
        scale = jnp.broadcast_to(scale1, (8, lanes))
        for i in range(tiles):
            at = pl.ds(i * 8, 8)
            once_ref[at, :] = start_ref[at, :] - inverse * (sens_ref[at, :] * scale)

        held_ref[...] = jnp.zeros(held_ref.shape, F32)
        factor = interface_weight * inverse
        edges = []
        for (d, b), start_b in zip(faces, starts):
            is_open = face_open(coords_ref, d, b)
            source = device_beyond(coords_ref, d, b)
            sent = in_ref[source].astype(F32)
            if d < 2:
                value = start_b[...] - (inverse * scale1) * sent[: (Y if d == 0 else X)]
                value = jnp.where(is_open, factor * value, 0.0)
                if d == 0:
                    x = face_position(coords_ref, d, b, X)
                    at = pl.ds(pl.multiple_of(x * Y, 8), Y)
                else:
                    at = pl.ds(face_position(coords_ref, d, b, Y), X, stride=Y)
                edges.append((at, value))
            else:
                for i in range(X * Y // lanes):
                    at = pl.ds(i * lanes, lanes)
                    value = start_b[pl.ds(0, 1), at] - (inverse * scale1) * sent[i : i + 1]
                    held_ref[pl.ds(b, 1), at] = jnp.where(is_open, factor * value, 0.0)
        out_ref[...] = spread_depth(turned_depth(held_ref[...]), coords_ref, (0, 1))
        for at, value in edges:
            out_ref[at, :] = out_ref[at, :] + value

        def body(x):
            for t in range(T):
                at = row(x, t)
                inside = valid(x, t)
                _, near_tiles = plain_neighbours(lambda x, t: once_ref[row(x, t), :], x, t)
                around = jnp.zeros((8, lanes), F32)
                for d in range(6):
                    around = around + jnp.where(inside[d], near_tiles[d], 0.0)
                p = phase_ref[at, :]
                drive = (
                    p / time_step
                    - 0.5 * p * (1.0 - p) * (1.0 - 2.0 * p)
                    - sens_ref[at, :] * scale
                )
                out_ref[at, :] += (drive + interface_weight * around) * inverse

        half = X // 2
        for part in range(2):
            for x in range(part * half, (part + 1) * half):
                body(x)
            at = pl.ds(part * half * Y, half * Y)
            writes.append(
                pltpu.make_async_copy(out_ref.at[at], out_hbm.at[at], written.at[part])
            )
            writes[-1].start()
        for write in writes:
            write.wait()

    phase_next, sensitivity = call(
        sweep_kernel,
        [(coords, SM), (incoming, VM), (sens_field, VM), (start, VM), (phase_f, VM)]
        + [(a, VM) for a in start_halo],
        [(plain_shape, F32, HB), (plain_shape, F32, HB)],
        scratch=[
            pltpu.VMEM(plain_shape, F32),
            pltpu.VMEM(plain_shape, F32),
            pltpu.VMEM((8, X * Y), F32),
            pltpu.SemaphoreType.DMA((3,)),
        ],
    )
    return (
        displacement.reshape(load.shape),
        sensitivity.reshape(phase.shape),
        phase_next.reshape(phase.shape),
    )


def solution(mesh):
    return program(mesh)


def program(mesh):
    return jax.shard_map(
        local,
        mesh=mesh,
        in_specs=(
            P(None, "span", "height", "depth"),
            P("span", "height", "depth"),
            P("span", "height", "depth"),
            P("span", "height", "depth"),
            P(("span", "height", "depth"), None, None),
        ),
        out_specs=(
            P(None, "span", "height", "depth"),
            P("span", "height", "depth"),
            P("span", "height", "depth"),
        ),
        check_vma=False,
    )
```

```python
import jax
import jax.numpy as jnp
from jax import lax
from jax.experimental import pallas as pl
from jax.experimental.pallas import tpu as pltpu
from jax.sharding import PartitionSpec as P


BE = 8
AXES = ("span", "height", "depth")

void_stiffness = 0.001
spring_rate = 0.05
time_step = 0.5
interface_weight = 0.5
epsilon_peak = 1e-06
inverse = 1.0 / (1.0 / time_step + 6.0 * interface_weight)

F32 = jnp.float32
BF16 = jnp.bfloat16
VM = pl.BlockSpec(memory_space=pltpu.VMEM)
SM = pl.BlockSpec(memory_space=pltpu.SMEM)


HB = pl.BlockSpec(memory_space=pltpu.HBM)


def call(kernel, ins, outs, scratch=(), flops=0, aliases=None):
    arrays = [
        pltpu.with_memory_space_constraint(
            array, pltpu.HBM if spec is HB else pltpu.SMEM if spec is SM else pltpu.VMEM
        )
        for array, spec in ins
    ]
    return pl.pallas_call(
        kernel,
        in_specs=[spec for _, spec in ins],
        out_specs=[spec for _, _, spec in outs],
        out_shape=[
            jax.ShapeDtypeStruct(shape, dtype)
            if spec is HB
            else (pltpu.SMEM if spec is SM else pltpu.VMEM)(shape, dtype)
            for shape, dtype, spec in outs
        ],
        scratch_shapes=list(scratch),
        input_output_aliases=aliases or {},
        cost_estimate=pl.CostEstimate(flops=flops, bytes_accessed=1 << 20, transcendentals=0),
        compiler_params=pltpu.CompilerParams(vmem_limit_bytes=12 << 20),
    )(*arrays)


def slots_fit(bricks, cells):
    return all(n * BE == size for n, size in zip(bricks, cells))


def local(load, phase, void, owner, precond):
    loads, X, Y, Z = load.shape
    bricks_x, bricks_y, bricks_z = void.shape
    bricks = bricks_x * bricks_y * bricks_z
    T = Y // BE
    tiles = X * T
    cells = BE**3
    lanes = Z
    assert lanes == 128 and BE == 8 and loads == 8 and slots_fit(void.shape, phase.shape)
    sizes = [lax.axis_size(axis) for axis in AXES]
    assert all(size % 2 == 0 for size in sizes)
    spans = sizes[0]
    devices = sizes[0] * sizes[1] * sizes[2]
    slots = precond.shape[0]
    cap = slots // spans
    bits = 32 // spans
    assert cap < (1 << min(bits, 8)) and bits >= 2
    remote = (spans - 1) * cap

    has_b = [size > 2 for size in sizes]
    faces = [(d, b) for d in range(3) for b in range(2) if b == 0 or has_b[d]]
    load_f = load.reshape(loads, X * Y, Z)
    phase_f = phase.reshape(X * Y, Z)

    def iotas():
        return (
            lax.broadcasted_iota(jnp.int32, (8, lanes), 0),
            lax.broadcasted_iota(jnp.int32, (8, lanes), 1),
        )

    def row(x, t):
        start = x * Y + t * 8
        return pl.ds(start if isinstance(start, int) else pl.multiple_of(start, 8), 8)

    def brick_at(n):
        m = jnp.maximum(n, 0)
        return m // (bricks_y * bricks_z), (m // bricks_z) % bricks_y, m % bricks_z

    def spread_of(rows, columns, row_part, column_part):
        r = lax.broadcasted_iota(jnp.int32, (rows, columns), 0)
        c = lax.broadcasted_iota(jnp.int32, (rows, columns), 1)
        same = jnp.logical_and(row_part(r) == column_part(c), (r & 7) == (c & 7))
        return jnp.where(same, 1.0, 0.0).astype(BF16)

    def halves(value):
        high = value.astype(BF16).astype(F32)
        return high, value - high

    def in_groups(count, one, group=4):
        while count % group:
            group //= 2

        def several(i, carry):
            for j in range(group):
                one(i * group + j)
            return carry

        lax.fori_loop(0, count // group, several, 0)

    def gather_bricks(source, table, base, count, out, group=4):
        sub, lane = iotas()
        keep = ((lane >> 3) & 7) == sub
        fold = spread_of(2 * lanes, lanes, lambda r: r >> 7, lambda c: c >> 6)
        pick = jnp.where(
            lax.broadcasted_iota(jnp.int32, (loads, loads * 8), 1) >> 3
            == lax.broadcasted_iota(jnp.int32, (loads, loads * 8), 0),
            1.0,
            0.0,
        ).astype(BF16)

        def one(r):
            n = table[base + r]
            bx, by, bz = brick_at(n)
            inside = (lane >> 3) == jnp.where(n >= 0, bz, -1)
            rows = []
            for q in range(4):
                for l in range(loads):
                    pair = [
                        jnp.where(inside, source[l, row(bx * 8 + 2 * q + h, by), :], 0.0)
                        for h in range(2)
                    ]
                    rows.append(jnp.concatenate(pair, axis=1))
            stacked = jnp.concatenate(rows, axis=0).astype(BF16)
            folded = jnp.dot(stacked, fold, preferred_element_type=F32)
            columns = []
            for q in range(4):
                columns.append(
                    jnp.concatenate(
                        [
                            jnp.where(
                                keep,
                                folded[(q * loads + l) * 8 : (q * loads + l + 1) * 8],
                                0.0,
                            )
                            for l in range(loads)
                        ],
                        axis=0,
                    )
                )
            cells_of = jnp.concatenate(columns, axis=1).astype(BF16)
            out[r] = jnp.dot(pick, cells_of, preferred_element_type=F32).astype(BF16)

        in_groups(count, one, group)

    def scatter_bricks(field, table, base, count, images, split):
        sub, lane = iotas()
        keep = ((lane >> 3) & 7) == sub
        unfold = spread_of(
            2 * lanes, 2 * lanes, lambda r: (r >> 6) & 1, lambda c: c >> 7
        )

        def one(r):
            n = table[base + r]
            bx, by, bz = brick_at(n)
            inside = (lane >> 3) == jnp.where(n >= 0, bz, -1)
            high, low = halves(images[r].astype(F32))
            split[r, 0] = high
            split[r, 1] = low
            rows = []
            for q in range(4):
                for l in range(loads):
                    pair = [
                        jnp.where(
                            keep,
                            jnp.broadcast_to(
                                split[r, part, pl.ds(l, 1), pl.ds(q * lanes, lanes)],
                                (8, lanes),
                            ),
                            0.0,
                        )
                        for part in range(2)
                    ]
                    rows.append(jnp.concatenate(pair, axis=1))
            stacked = jnp.concatenate(rows, axis=0).astype(BF16)
            spread = jnp.dot(stacked, unfold, preferred_element_type=F32)
            for q in range(4):
                for l in range(loads):
                    for h in range(2):
                        at = row(bx * 8 + 2 * q + h, by)
                        tile = spread[
                            (q * loads + l) * 8 : (q * loads + l + 1) * 8,
                            h * lanes : (h + 1) * lanes,
                        ]
                        field[l, at, :] = jnp.where(inside, tile, field[l, at, :])

        in_groups(count, one)

    def face_position(coords_ref, d, b, extent):
        high = (coords_ref[d] + b) % 2 == 0
        return jnp.where(high, extent - 1, 0)

    def face_open(coords_ref, d, b):
        if b == 0:
            return jnp.bool_(True)
        return jnp.logical_and(coords_ref[d] > 0, coords_ref[d] < sizes[d] - 1)

    def put_faces(read_tile, read_rows, coords_ref, index, outs):
        for (d, b), out in zip(faces, outs):
            if d == 0:
                x = face_position(coords_ref, d, b, X)
                for t in range(T):
                    out[index, pl.ds(t * 8, 8), :] = read_tile(x, t).astype(out.dtype)
            elif d == 1:
                out[index] = read_rows(face_position(coords_ref, d, b, Y)).astype(out.dtype)

    def depth_faces(fields, coords_ref, count, addends=2):
        rows_i = lax.broadcasted_iota(jnp.int32, (2 * count, lanes), 0)
        lanes_i = lax.broadcasted_iota(jnp.int32, (2 * count, lanes), 1)
        z = [face_position(coords_ref, 2, b, lanes) for b in range(2)]
        total = jnp.zeros((2 * count, X * Y), F32)
        for f, field in enumerate(fields):
            hit = [
                jnp.logical_and(rows_i == b * count + f, lanes_i == z[b]) for b in range(2)
            ]
            pick = jnp.where(jnp.logical_or(*hit), 1.0, 0.0).astype(BF16)
            for part in halves(field())[:addends]:
                total = total + lax.dot_general(
                    pick,
                    part.astype(BF16),
                    (((1,), (1,)), ((), ())),
                    preferred_element_type=F32,
                )
        return total

    def turned_depth(values):
        return jnp.transpose(jnp.concatenate(halves(values), axis=0)).astype(BF16)

    def spread_depth(turned, coords_ref, rows_of):
        total = turned.shape[1] // 2
        rows_i = lax.broadcasted_iota(jnp.int32, (2 * total, lanes), 0) % total
        lanes_i = lax.broadcasted_iota(jnp.int32, (2 * total, lanes), 1)
        hit = [
            jnp.logical_and(
                rows_i == rows_of[b], lanes_i == face_position(coords_ref, 2, b, lanes)
            )
            for b in range(2)
        ]
        place = jnp.where(jnp.logical_or(*hit), 1.0, 0.0).astype(BF16)
        return jnp.dot(turned, place, preferred_element_type=F32)

    def plain_neighbours(read, x, t):
        sub, _ = iotas()
        tile = read(x, t)
        x_low = read(jnp.maximum(x - 1, 0), t)
        x_high = read(jnp.minimum(x + 1, X - 1), t)
        before = jnp.where(sub == 7, read(x, t - 1), tile) if t > 0 else tile
        after = jnp.where(sub == 0, read(x, t + 1), tile) if t < T - 1 else tile
        return tile, (
            x_low,
            x_high,
            pltpu.roll(before, 1, 0),
            pltpu.roll(after, 7, 0),
            pltpu.roll(tile, 1, 1),
            pltpu.roll(tile, lanes - 1, 1),
        )

    def valid(x, t):
        sub, lane = iotas()
        yes = sub >= 0
        return (
            jnp.logical_and(yes, x > 0),
            jnp.logical_and(yes, x < X - 1),
            sub > 0 if t == 0 else yes,
            sub < 7 if t == T - 1 else yes,
            lane > 0,
            lane < lanes - 1,
        )

    def over_rows(body, group=2):
        def several(i, carry):
            for j in range(group):
                body(i * group + j)
            return carry

        lax.fori_loop(0, X // group, several, 0)

    def face_shape(d, count):
        return ((count, Y, Z), (count, X, Z), (-(-count // 8) * 8, X * Y))[d]

    def face_outs(count, dtype):
        return [(face_shape(d, count), dtype, VM) for d, _ in faces]

    def exchange(payload):
        received = [None] * len(faces)
        for (d, b), part in zip(faces, payload):
            n = sizes[d]
            swap = [(i, (i + 1 if (i + b) % 2 == 0 else i - 1) % n) for i in range(n)]
            received[faces.index((d, b))] = lax.ppermute(part, AXES[d], swap)
        return received

    def to_owners(rows, sign):
        parts = []
        for shift in range(1, spans):
            part = rows[(shift - 1) * cap : shift * cap]
            parts.append(
                lax.ppermute(
                    part, "span", [(i, (i + sign * shift) % spans) for i in range(spans)]
                )
            )
        return parts[0] if spans == 2 else jnp.concatenate(parts, axis=0)

    def everyone(partial):
        return lax.all_to_all(partial, AXES, split_axis=0, concat_axis=0, tiled=True)

    field_shape = (loads, X * Y, Z)
    plain_shape = (X * Y, Z)
    face_count = len(faces)

    def first_kernel(
        void_hbm, owner_hbm, load_hbm, phase_hbm, blocks_hbm,
        table_ref, far_ref, load_ref, phase_ref, blocks_ref, coords_ref, void_ref,
        owner_ref, arrived,
    ):
        me = lax.axis_index("span")
        copies = [
            pltpu.make_async_copy(source, target, arrived.at[i])
            for i, (source, target) in enumerate(
                (
                    (void_hbm, void_ref),
                    (owner_hbm, owner_ref),
                    (load_hbm, load_ref),
                    (phase_hbm, phase_ref),
                    (blocks_hbm.at[pl.ds(me * cap, cap)], blocks_ref),
                )
            )
        ]
        for copy in copies:
            copy.start()
        for d, axis in enumerate(AXES):
            coords_ref[d] = lax.axis_index(axis)
        for i in range(slots + 1):
            table_ref[i] = -1
        copies[0].wait()
        copies[1].wait()
        used = jnp.int32(0)
        for n in range(bricks):
            at = (n // (bricks_y * bricks_z), n // bricks_z % bricks_y, n % bricks_z)
            solid = 1 - void_ref[at]
            relative = jnp.where(solid == 1, (owner_ref[at] + spans - me) % spans, 0)
            shift = relative * bits
            rank = lax.shift_right_logical(used, shift) & ((1 << bits) - 1)
            index = jnp.where(solid == 1, relative * cap + rank, slots)
            table_ref[index] = n
            used = used + lax.shift_left(solid, shift)
        copies[2].wait()
        gather_bricks(load_ref, table_ref, cap, remote, far_ref, group=8)
        copies[3].wait()
        copies[4].wait()

    table, far, load_f, phase_f, near_blocks, coords, void = pl.pallas_call(
        first_kernel,
        in_specs=[HB] * 5,
        out_specs=[SM, VM, VM, VM, VM, SM, SM],
        out_shape=[
            pltpu.SMEM((slots + 1,), jnp.int32),
            pltpu.VMEM((remote, loads, cells), BF16),
            pltpu.VMEM(field_shape, F32),
            pltpu.VMEM(plain_shape, F32),
            pltpu.VMEM((cap, cells, cells), BF16),
            pltpu.SMEM((3,), jnp.int32),
            pltpu.SMEM(void.shape, jnp.int32),
        ],
        scratch_shapes=[
            pltpu.SMEM(owner.shape, jnp.int32),
            pltpu.SemaphoreType.DMA((5,)),
        ],
        compiler_params=pltpu.CompilerParams(vmem_limit_bytes=12 << 20),
        name="first",
    )(*[
        pltpu.with_memory_space_constraint(a, pltpu.HBM)
        for a in (void, owner, load_f, phase_f, precond)
    ])

    def near_kernel(bring):
        def kernel(table_ref, coords_ref, source_ref, blocks_ref, *refs):
            copies = []
            if bring:
                hbm, field_ref, far_ref, rows_ref, image_ref, split, arrived = refs
                for shift in range(1, spans):
                    source = (coords_ref[0] + spans - shift) % spans
                    copies.append(
                        pltpu.make_async_copy(
                            hbm.at[pl.ds(source * cap, cap)],
                            far_ref.at[pl.ds((shift - 1) * cap, cap)],
                            arrived.at[shift - 1],
                        )
                    )
                    copies[-1].start()
            else:
                field_ref, rows_ref, image_ref, split = refs
            field_ref[...] = jnp.zeros(field_ref.shape, F32)
            gather_bricks(source_ref, table_ref, 0, cap, rows_ref)
            for r in range(cap):
                image_ref[r] = jnp.dot(
                    rows_ref[r], blocks_ref[r], preferred_element_type=F32
                )
            scatter_bricks(field_ref, table_ref, 0, cap, image_ref, split)
            for copy in copies:
                copy.wait()

        return kernel

    def near_part(source, bring):
        ins = [(table, SM), (coords, SM), (source, VM), (near_blocks, VM)]
        outs = [(field_shape, F32, VM)]
        scratch = [
            pltpu.VMEM((cap, loads, cells), BF16),
            pltpu.VMEM((cap, loads, cells), F32),
            pltpu.VMEM((cap, 2, loads, cells), F32),
        ]
        if bring:
            ins.append((precond, HB))
            outs.append(((remote, cells, cells), BF16, VM))
            scratch.append(pltpu.SemaphoreType.DMA((spans - 1,)))
        return call(near_kernel(bring), ins, outs, scratch=scratch, flops=8000000000)

    def blocks_kernel(rows_ref, blocks_ref, out_ref):
        for r in range(remote):
            out_ref[r] = jnp.dot(
                rows_ref[r], blocks_ref[r], preferred_element_type=F32
            ).astype(out_ref.dtype)

    def far_part(rows, dtype):
        (image,) = call(
            blocks_kernel,
            [(to_owners(rows, 1), VM), (far_blocks, VM)],
            [((remote, loads, cells), dtype, VM)],
        )
        return to_owners(image, -1)

    def faces_kernel(extra):
        def kernel(table_ref, coords_ref, image_ref, begun_ref, *refs):
            extras = refs[:extra]
            field_ref = refs[extra]
            outs = refs[extra + 1 : extra + 1 + face_count]
            split = refs[extra + 1 + face_count]
            scatter_bricks(field_ref, table_ref, cap, remote, image_ref, split)
            for l in range(loads):
                put_faces(
                    lambda x, t: field_ref[l, row(x, t), :],
                    lambda y: field_ref[l, pl.ds(y, X, stride=Y), :],
                    coords_ref, l, outs,
                )
            for e in range(extra):
                ref = extras[e]
                put_faces(
                    lambda x, t: ref[row(x, t), :],
                    lambda y: ref[pl.ds(y, X, stride=Y), :],
                    coords_ref, loads + e, outs,
                )
            count = outs[-1].shape[0]
            depth = depth_faces(
                [lambda l=l: field_ref[l] for l in range(loads)]
                + [lambda e=e: extras[e][...] for e in range(extra)],
                coords_ref, count, addends=1,
            )
            for (d, b), out in zip(faces, outs):
                if d == 2:
                    out[...] = depth[b * count : (b + 1) * count].astype(out.dtype)

        return kernel

    def to_field(begun, image, extras, dtype):
        result = call(
            faces_kernel(len(extras)),
            [(table, SM), (coords, SM), (image, VM), (begun, VM)]
            + [(e, VM) for e in extras],
            [(field_shape, F32, VM)] + face_outs(loads + len(extras), dtype),
            scratch=[pltpu.VMEM((remote, 2, loads, cells), F32)],
            aliases={3: 0},
        )
        return result[0], result[1:], exchange(result[1:])

    def stiffness_kernel(void_ref, phase_ref, ks_ref):
        _, lane = iotas()
        for bx in range(bricks_x):
            for by in range(bricks_y):
                mask = jnp.zeros((8, lanes), F32)
                for bz in range(bricks_z):
                    solid = 1 - void_ref[bx, by, bz]
                    mask = jnp.where((lane >> 3) == bz, solid.astype(F32), mask)
                for i in range(BE):
                    at = row(bx * BE + i, by)
                    p = phase_ref[at, :]
                    stiffness = void_stiffness + (1.0 - void_stiffness) * (p * p * p)
                    ks_ref[at, :] = mask * stiffness

    begun, far_blocks = near_part(load_f, True)
    far_image = far_part(far, F32)
    (ks,) = call(
        stiffness_kernel, [(void, SM), (phase_f, VM)], [(plain_shape, F32, VM)],
        flops=2000000000,
    )
    z_field, z_sent, z_halo = to_field(begun, far_image, [ks, phase_f], F32)

    def joined(mine, other):
        both = jnp.logical_and(mine > 0.0, other > 0.0)
        return jnp.where(both, 0.5 * (mine + other), 0.0)

    def inner_kernel(z_ref, load_ref, ks_ref, phase_ref, q_ref, weight_ref, start_ref, dots_ref):
        dots_ref[...] = jnp.zeros(dots_ref.shape, F32)

        def body(x):
            for t in range(T):
                at = row(x, t)
                inside = valid(x, t)
                ks_tile, ks_near = plain_neighbours(lambda x, t: ks_ref[row(x, t), :], x, t)
                p, p_near = plain_neighbours(lambda x, t: phase_ref[row(x, t), :], x, t)
                around = jnp.zeros((8, lanes), F32)
                for d in range(6):
                    around = around + jnp.where(inside[d], p_near[d], 0.0)
                start_ref[at, :] = (
                    p / time_step
                    - 0.5 * p * (1.0 - p) * (1.0 - 2.0 * p)
                    + interface_weight * around
                ) * inverse
                total = jnp.where(ks_tile > 0.0, spring_rate, 0.0)
                weights = []
                for d in range(6):
                    weight = jnp.where(inside[d], joined(ks_tile, ks_near[d]), 0.0)
                    weights.append(weight)
                    weight_ref[d, at, :] = weight
                    total = total + weight
                for l in range(loads):
                    tile, near_tiles = plain_neighbours(
                        lambda x, t: z_ref[l, row(x, t), :], x, t
                    )
                    image = total * tile
                    for d in range(6):
                        image = image - weights[d] * near_tiles[d]
                    q_ref[l, at, :] = image
                    dots_ref[0, l] += load_ref[l, at, :] * tile
                    dots_ref[1, l] += image * tile

        over_rows(body)

    q_inner, weights, start_inner, dots = call(
        inner_kernel,
        [(z_field, VM), (load_f, VM), (ks, VM), (phase_f, VM)],
        [
            (field_shape, F32, VM),
            ((6, X * Y, Z), F32, VM),
            (plain_shape, F32, VM),
            ((2, loads, 8, Z), F32, VM),
        ],
        flops=8000000000,
    )

    def face_weight(coords_ref, d, b, sent, received, at):
        other = jnp.where(face_open(coords_ref, d, b), received[at], 0.0)
        return joined(sent[at], other)

    def row_pieces(d):
        return [pl.ds(i * 8, 8) for i in range((Y if d == 0 else X) // 8)]

    def edges_kernel(coords_ref, table_ref, q_in, start_in, dots_in, *refs):
        sent = refs[:face_count]
        received = refs[face_count : 2 * face_count]
        q_ref, start_ref, dots_ref, far_ref = refs[2 * face_count : 2 * face_count + 4]
        moved = refs[2 * face_count + 4 :]
        scale = interface_weight * inverse
        for (d, b), mine, other, shift in zip(faces, sent, received, moved):
            is_open = face_open(coords_ref, d, b)
            if d < 2:
                for at in row_pieces(d):
                    weight = face_weight(coords_ref, d, b, mine, other, (loads, at))
                    for l in range(loads):
                        tile = mine[l, at, :]
                        change = weight * (tile - other[l, at, :])
                        shift[l, at, :] = change
                        dots_ref[1, l] += tile * change
                    shift[loads, at, :] = jnp.where(
                        is_open, scale * other[loads + 1, at, :], 0.0
                    )
                for l in range(loads + 1):
                    target = q_ref.at[l] if l < loads else start_ref
                    if d == 0:
                        x = face_position(coords_ref, d, b, X)
                        for t in range(T):
                            target[row(x, t), :] += shift[l, pl.ds(t * 8, 8), :]
                    else:
                        y = face_position(coords_ref, d, b, Y)
                        at = pl.ds(y, X, stride=Y)
                        target[at, :] = target[at, :] + shift[l]
            else:
                weight = face_weight(coords_ref, d, b, mine, other, (pl.ds(loads, 1), slice(None)))
                tile = mine[pl.ds(0, loads), :]
                change = weight * (tile - other[pl.ds(0, loads), :])
                shift[pl.ds(0, loads), :] = change
                shift[pl.ds(loads, 8), :] = jnp.zeros((8, X * Y), F32)
                shift[pl.ds(loads, 1), :] = jnp.where(
                    is_open, scale * other[pl.ds(loads + 1, 1), :], 0.0
                )
                product = tile * change
                eight = sum(
                    product[:, i * lanes : (i + 1) * lanes] for i in range(X * Y // lanes)
                )
                sub, _ = iotas()
                for l in range(loads):
                    dots_ref[1, l] += jnp.where(sub == l, eight, 0.0)
        depth = [shift for (d, _), shift in zip(faces, moved) if d == 2]
        turned = turned_depth(jnp.concatenate([ref[...] for ref in depth], axis=0))
        for l in range(loads + 1):
            target = q_ref.at[l] if l < loads else start_ref
            target[...] = target[...] + spread_depth(
                turned, coords_ref, (l, depth[0].shape[0] + l)
            )
        gather_bricks(q_ref, table_ref, cap, remote, far_ref)

    q_field, start, dots, far = call(
        edges_kernel,
        [(coords, SM), (table, SM), (q_inner, VM), (start_inner, VM), (dots, VM)]
        + [(a, VM) for a in z_sent]
        + [(a, VM) for a in z_halo],
        [
            (field_shape, F32, VM),
            (plain_shape, F32, VM),
            ((2, loads, 8, Z), F32, VM),
            ((remote, loads, cells), BF16, VM),
        ],
        scratch=[pltpu.VMEM(face_shape(d, loads + 1), F32) for d, _ in faces],
        aliases={2: 0, 3: 1, 4: 2},
    )

    far_image = far_part(far, BF16)
    w_field, w_sent, w_halo = to_field(
        near_part(q_field, False)[0], far_image, [start], BF16
    )

    products = 5

    def more_kernel(w_ref, q_ref, load_ref, weight_ref, ks_ref, more_ref):
        more_ref[...] = jnp.zeros(more_ref.shape, F32)

        def body(x):
            for t in range(T):
                at = row(x, t)
                weights = [weight_ref[d, at, :] for d in (1, 3, 5)]
                spring = jnp.where(ks_ref[at, :] > 0.0, spring_rate, 0.0)
                for l in range(loads):
                    tile, near_tiles = plain_neighbours(
                        lambda x, t: w_ref[l, row(x, t), :], x, t
                    )
                    energy = spring * tile * tile
                    for weight, d in zip(weights, (1, 3, 5)):
                        gap = tile - near_tiles[d]
                        energy = energy + weight * gap * gap
                    more_ref[0, l] += load_ref[l, at, :] * tile
                    more_ref[1, l] += q_ref[l, at, :] * tile
                    more_ref[2, l] += energy

        over_rows(body)

    (more,) = call(
        more_kernel,
        [(w_field, VM), (q_field, VM), (load_f, VM), (weights, VM), (ks, VM)],
        [((3, loads, 8, Z), F32, VM)],
        flops=8000000000,
    )

    def total_kernel(coords_ref, dots_ref, more_in, *refs):
        z_mine = refs[:face_count]
        z_other = refs[face_count : 2 * face_count]
        w_mine = refs[2 * face_count : 3 * face_count]
        w_other = refs[3 * face_count : 4 * face_count]
        out_ref, more_ref = refs[4 * face_count : 4 * face_count + 2]
        gaps = refs[4 * face_count + 2 : 5 * face_count + 2]
        starts = refs[5 * face_count + 2 :]
        sub, lane = iotas()
        for (d, b), z_a, z_b, w_a, w_b, gap, begin in zip(
            faces, z_mine, z_other, w_mine, w_other, gaps, starts
        ):
            if d < 2:
                begin[...] = w_b[loads].astype(F32)
                for at in row_pieces(d):
                    weight = face_weight(coords_ref, d, b, z_a, z_b, (loads, at))
                    solid = weight > 0.0
                    for l in range(loads):
                        tile = w_a[l, at, :].astype(F32)
                        between = tile - w_b[l, at, :].astype(F32)
                        more_ref[2, l] += weight * tile * between
                        gap[1, l, at, :] = jnp.where(solid, between, 0.0)
                        gap[0, l, at, :] = jnp.where(
                            solid, z_a[l, at, :] - z_b[l, at, :], 0.0
                        )
            else:
                begin[...] = w_b[...].astype(F32)[loads : loads + 8]
                weight = face_weight(coords_ref, d, b, z_a, z_b, (pl.ds(loads, 1), slice(None)))
                solid = weight > 0.0
                tile = w_a[...].astype(F32)[:loads]
                between = tile - w_b[...].astype(F32)[:loads]
                product = weight * tile * between
                gap[1] = jnp.where(solid, between, 0.0)
                gap[0] = jnp.where(
                    solid, z_a[pl.ds(0, loads), :] - z_b[pl.ds(0, loads), :], 0.0
                )
                eight = sum(
                    product[:, i * lanes : (i + 1) * lanes] for i in range(X * Y // lanes)
                )
                for l in range(loads):
                    more_ref[2, l] += jnp.where(sub == l, eight, 0.0)
        result = jnp.zeros((1, lanes), F32)
        lane1 = lane[:1]
        for k in range(products):
            for l in range(loads):
                part = dots_ref[k, l] if k < 2 else more_ref[k - 2, l]
                value = jnp.sum(jnp.sum(part, axis=0, keepdims=True), axis=1, keepdims=True)
                result = jnp.where(lane1 == k * loads + l, value, result)
        out_ref[...] = jnp.broadcast_to(result, (devices, lanes))

    partial, _, *kept = call(
        total_kernel,
        [(coords, SM), (dots, VM), (more, VM)]
        + [(a, VM) for part in (z_sent, z_halo, w_sent, w_halo) for a in part],
        [((devices, lanes), F32, VM), ((3, loads, 8, Z), F32, VM)]
        + [((2,) + face_shape(d, loads), F32, VM) for d, _ in faces]
        + [((8, X * Y) if d == 2 else face_shape(d, 1)[1:], F32, VM) for d, _ in faces],
        aliases={2: 1},
    )
    gaps, start_halo = kept[:face_count], kept[face_count:]
    sums = everyone(partial)

    def device_beyond(coords_ref, d, b):
        place = [coords_ref[i] for i in range(3)]
        step = jnp.where((place[d] + b) % 2 == 0, 1, -1)
        place[d] = jnp.where(face_open(coords_ref, d, b), place[d] + step, place[d])
        return (place[0] * sizes[1] + place[1]) * sizes[2] + place[2]

    face_rows = max(X, Y)
    message = face_rows + 1

    def solve_kernel(
        coords_ref, sums_ref, ks_ref, phase_ref, z_ref, w_ref, *refs
    ):
        gap_refs = refs[:face_count]
        sens_ref, out_ref, x_hbm, x_ref, plain_ref, link_ref, held_ref, written = refs[
            face_count:
        ]
        sub, lane = iotas()
        total = jnp.broadcast_to(
            jnp.sum(sums_ref[...], axis=0, keepdims=True), (8, lanes)
        )
        bz, zq, bw, qw, ws = [
            pltpu.roll(total, (lanes - k * loads) % lanes, 1) for k in range(products)
        ]
        alpha = bz / zq
        bz_next = bz - alpha * (bw + zq) + alpha * alpha * qw
        beta = bz_next / bz
        grow = 1.0 + beta
        curvature = grow * grow * zq - 2.0 * grow * alpha * qw + alpha * alpha * ws
        alpha_next = bz_next / curvature
        for_z = alpha + alpha_next * grow
        for_w = -alpha_next * alpha
        c_z = [jnp.broadcast_to(for_z[0:1, l : l + 1], (8, lanes)) for l in range(loads)]
        c_w = [jnp.broadcast_to(for_w[0:1, l : l + 1], (8, lanes)) for l in range(loads)]
        writes = []
        for l in range(loads):
            for i in range(tiles):
                at = pl.ds(i * 8, 8)
                x_ref[l, at, :] = c_z[l] * z_ref[l, at, :] + c_w[l] * w_ref[l, at, :]
            writes.append(
                pltpu.make_async_copy(x_ref.at[l], x_hbm.at[l], written.at[l])
            )
            writes[-1].start()

        def body(x):
            for t in range(T):
                at = row(x, t)
                inside = valid(x, t)
                ks_tile, ks_near = plain_neighbours(lambda x, t: ks_ref[row(x, t), :], x, t)
                gaps_of = [jnp.zeros((8, lanes), F32) for _ in range(3)]
                for l in range(loads):
                    tile, near_tiles = plain_neighbours(
                        lambda x, t: x_ref[l, row(x, t), :], x, t
                    )
                    for d in range(3):
                        gap = tile - near_tiles[2 * d + 1]
                        gaps_of[d] = gaps_of[d] + gap * gap
                for d in range(3):
                    n = 2 * d + 1
                    solid = jnp.logical_and(inside[n], joined(ks_tile, ks_near[n]) > 0.0)
                    link_ref[d, at, :] = jnp.where(solid, gaps_of[d], 0.0)

        over_rows(body)
        for x in range(X):
            for t in range(T):
                at = row(x, t)
                along_y = link_ref[1, at, :]
                before = link_ref[1, row(x, t - 1), :] if t > 0 else 0.0
                along_z = link_ref[2, at, :]
                energy = link_ref[0, at, :] + along_y + along_z
                energy = energy + pltpu.roll(jnp.where(sub == 7, before, along_y), 1, 0)
                energy = energy + pltpu.roll(along_z, 1, 1)
                if x > 0:
                    energy = energy + link_ref[0, row(x - 1, t), :]
                plain_ref[at, :] = energy
        held_ref[...] = jnp.zeros(held_ref.shape, F32)
        for (d, b), between in zip(faces, gap_refs):
            if d < 2:
                pieces = []
                for at in row_pieces(d):
                    energy = jnp.zeros((8, lanes), F32)
                    for l in range(loads):
                        gap = c_z[l] * between[0, l, at, :] + c_w[l] * between[1, l, at, :]
                        energy = energy + gap * gap
                    pieces.append(energy)
                if d == 0:
                    x = face_position(coords_ref, d, b, X)
                    for t in range(T):
                        plain_ref[row(x, t), :] += pieces[t]
                else:
                    at = pl.ds(face_position(coords_ref, d, b, Y), X, stride=Y)
                    plain_ref[at, :] = plain_ref[at, :] + jnp.concatenate(pieces, axis=0)
            else:
                by_z = jnp.concatenate([c[0:1, :1] for c in c_z], axis=0)
                by_w = jnp.concatenate([c[0:1, :1] for c in c_w], axis=0)
                gap = by_z * between[0] + by_w * between[1]
                held_ref[pl.ds(b, 1), :] = jnp.sum(gap * gap, axis=0, keepdims=True)
        spread = spread_depth(turned_depth(held_ref[...]), coords_ref, (0, 1))
        energy = plain_ref[...] + spread
        p = phase_ref[...]
        negative = 1.5 * (1.0 - void_stiffness) * (p * p) * energy
        sens_ref[...] = -negative
        peak = jnp.max(jnp.max(negative, axis=0, keepdims=True), axis=1, keepdims=True)
        peak = jnp.broadcast_to(peak, (1, lanes))
        high, rest = halves(peak)
        middle, low = halves(rest)
        lane1 = lane[:1]
        tail = jnp.where(lane1 == 0, high, jnp.where(lane1 == 1, middle, low)).astype(BF16)
        for i in range(devices):
            out_ref[i, pl.ds(face_rows, 1), :] = tail
        depth = depth_faces([lambda: sens_ref[...]], coords_ref, 8, addends=1)
        for d, b in faces:
            @pl.when(face_open(coords_ref, d, b))
            def _(d=d, b=b):
                to = device_beyond(coords_ref, d, b)
                if d == 0:
                    x = face_position(coords_ref, d, b, X)
                    value = sens_ref[pl.ds(pl.multiple_of(x * Y, 8), Y), :]
                elif d == 1:
                    value = sens_ref[
                        pl.ds(face_position(coords_ref, d, b, Y), X, stride=Y), :
                    ]
                else:
                    value = jnp.concatenate(
                        [
                            depth[b * 8 : b * 8 + 1, i * lanes : (i + 1) * lanes]
                            for i in range(X * Y // lanes)
                        ],
                        axis=0,
                    )
                out_ref[to, pl.ds(0, value.shape[0]), :] = value.astype(BF16)
        for write in writes:
            write.wait()

    sens_field, outgoing, displacement = call(
        solve_kernel,
        [
            (coords, SM), (sums, VM), (ks, VM), (phase_f, VM), (z_field, VM),
            (w_field, VM),
        ]
        + [(a, VM) for a in gaps],
        [
            (plain_shape, F32, VM),
            ((devices, message, lanes), BF16, VM),
            (field_shape, F32, HB),
        ],
        scratch=[
            pltpu.VMEM(field_shape, F32),
            pltpu.VMEM(plain_shape, F32),
            pltpu.VMEM((3,) + plain_shape, F32),
            pltpu.VMEM((8, X * Y), F32),
            pltpu.SemaphoreType.DMA((loads,)),
        ],
    )
    incoming = everyone(outgoing)

    def sweep_kernel(coords_ref, in_ref, sens_ref, start_ref, phase_ref, *refs):
        starts = refs[:face_count]
        out_hbm, sens_hbm, out_ref, once_ref, held_ref, written = refs[face_count:]
        writes = [pltpu.make_async_copy(sens_ref, sens_hbm, written.at[2])]
        writes[0].start()
        sub, lane = iotas()
        tails = in_ref[:, pl.ds(face_rows, 1), :].astype(F32)
        tails = tails.reshape(devices, lanes)
        peaks = tails + pltpu.roll(tails, lanes - 1, 1) + pltpu.roll(tails, lanes - 2, 1)
        peak = jnp.max(peaks, axis=0, keepdims=True)[:, :1]
        scale1 = jnp.broadcast_to(1.0 / (peak + epsilon_peak), (1, lanes))
        scale = jnp.broadcast_to(scale1, (8, lanes))
        for i in range(tiles):
            at = pl.ds(i * 8, 8)
            once_ref[at, :] = start_ref[at, :] - inverse * (sens_ref[at, :] * scale)

        held_ref[...] = jnp.zeros(held_ref.shape, F32)
        factor = interface_weight * inverse
        edges = []
        for (d, b), start_b in zip(faces, starts):
            is_open = face_open(coords_ref, d, b)
            source = device_beyond(coords_ref, d, b)
            sent = in_ref[source].astype(F32)
            if d < 2:
                value = start_b[...] - (inverse * scale1) * sent[: (Y if d == 0 else X)]
                value = jnp.where(is_open, factor * value, 0.0)
                if d == 0:
                    x = face_position(coords_ref, d, b, X)
                    at = pl.ds(pl.multiple_of(x * Y, 8), Y)
                else:
                    at = pl.ds(face_position(coords_ref, d, b, Y), X, stride=Y)
                edges.append((at, value))
            else:
                for i in range(X * Y // lanes):
                    at = pl.ds(i * lanes, lanes)
                    value = start_b[pl.ds(0, 1), at] - (inverse * scale1) * sent[i : i + 1]
                    held_ref[pl.ds(b, 1), at] = jnp.where(is_open, factor * value, 0.0)
        out_ref[...] = spread_depth(turned_depth(held_ref[...]), coords_ref, (0, 1))
        for at, value in edges:
            out_ref[at, :] = out_ref[at, :] + value

        def body(x):
            for t in range(T):
                at = row(x, t)
                inside = valid(x, t)
                _, near_tiles = plain_neighbours(lambda x, t: once_ref[row(x, t), :], x, t)
                around = jnp.zeros((8, lanes), F32)
                for d in range(6):
                    around = around + jnp.where(inside[d], near_tiles[d], 0.0)
                p = phase_ref[at, :]
                drive = (
                    p / time_step
                    - 0.5 * p * (1.0 - p) * (1.0 - 2.0 * p)
                    - sens_ref[at, :] * scale
                )
                out_ref[at, :] += (drive + interface_weight * around) * inverse

        half = X // 2
        for part in range(2):
            for x in range(part * half, (part + 1) * half):
                body(x)
            at = pl.ds(part * half * Y, half * Y)
            writes.append(
                pltpu.make_async_copy(out_ref.at[at], out_hbm.at[at], written.at[part])
            )
            writes[-1].start()
        for write in writes:
            write.wait()

    phase_next, sensitivity = call(
        sweep_kernel,
        [(coords, SM), (incoming, VM), (sens_field, VM), (start, VM), (phase_f, VM)]
        + [(a, VM) for a in start_halo],
        [(plain_shape, F32, HB), (plain_shape, F32, HB)],
        scratch=[
            pltpu.VMEM(plain_shape, F32),
            pltpu.VMEM(plain_shape, F32),
            pltpu.VMEM((8, X * Y), F32),
            pltpu.SemaphoreType.DMA((3,)),
        ],
    )
    return (
        displacement.reshape(load.shape),
        sensitivity.reshape(phase.shape),
        phase_next.reshape(phase.shape),
    )


def solution(mesh):
    return program(mesh)


def program(mesh):
    return jax.shard_map(
        local,
        mesh=mesh,
        in_specs=(
            P(None, "span", "height", "depth"),
            P("span", "height", "depth"),
            P("span", "height", "depth"),
            P("span", "height", "depth"),
            P(("span", "height", "depth"), None, None),
        ),
        out_specs=(
            P(None, "span", "height", "depth"),
            P("span", "height", "depth"),
            P("span", "height", "depth"),
        ),
        check_vma=False,
    )
```
